32 devices in a mesh: seq: 8 (over y, x, core), head: 4 (over z).
Axes of the slice: x: 2, y: 2, z: 4, core: 2. Of those that a mesh axis runs over, the one named last changes fastest.
Arguments:
- queries: bfloat16 [8192, 2048], P('seq', 'head'), may hold values from -6 to 6
- keys: bfloat16 [8192, 2048], P('seq', 'head'), may hold values from -100 to 100
- values: bfloat16 [8192, 2048], P('seq', 'head'), may hold values from -16 to 16
- gates: float32 [8192, 16], P('seq', 'head'), may hold values from 0.05 to 1
- ridge: float32 [16], P('head'), may hold values from 0.25 to 4
- out_weight: bfloat16 [2048, 2048], P(None, 'head'), may hold values from -0.125 to 0.125
Outputs:
- partial_out: bfloat16 [4, 8192, 2048], P('head', 'seq')
The draws below stay inside these ranges and needn't reach their ends.
All inputs are finite; a program needn't handle non-finite values.
Results may differ from the reference program's by a relative error of at most 0.0049.
Values may be sent and summed in bfloat16 or wider, within the bound.
A program may use at most 128 MiB of HBM per device.

```python
import math
import jax
import jax.numpy as jnp
from jax import lax

D = 2048
HEADS = 16
HD = 128
SPAN = 128
ITERS = 8
TOKENS = 8192
N_HEAD = 4


def key_value_pair(key):
    scale_key = jax.random.fold_in(key, 101)
    normal_key = jax.random.fold_in(key, 202)
    mixing_key = jax.random.fold_in(key, 303)
    noise_key = jax.random.fold_in(key, 404)
    columns = HEADS * HD
    spread = math.log(10.0)
    scales = jnp.exp(jax.random.uniform(scale_key, (columns,), jnp.float32, 0.0, spread))
    base = jax.random.normal(normal_key, (TOKENS, columns), jnp.float32)
    raw_keys = jnp.clip(base * scales, -100.0, 100.0)
    grouped = raw_keys.reshape(TOKENS, HEADS, HD)
    unit_keys = grouped * lax.rsqrt(jnp.sum(grouped * grouped, -1, keepdims=True) + 1e-06)
    mixing = jax.random.normal(mixing_key, (HEADS, HD, HD), jnp.float32)
    mapped = jnp.einsum('thd,hde->the', unit_keys, mixing)
    noisy = mapped + 0.7 * jax.random.normal(noise_key, (TOKENS, HEADS, HD), jnp.float32)
    return (raw_keys, jnp.clip(noisy, -16.0, 16.0).reshape(TOKENS, columns))


def draw_keys(key, part):
    return key_value_pair(key)[0].astype(jnp.bfloat16)


def draw_values(key, part):
    return key_value_pair(key)[1].astype(jnp.bfloat16)


def block_scale(rng, shape, pieces, least, high):
    gain, own = 1.0, jax.random.fold_in(rng, 6)
    for axis_at, shards_of in pieces:
        heights = jnp.exp(jax.random.uniform(jax.random.fold_in(own, axis_at), (shards_of,), jnp.float32, least / len(pieces), high / len(pieces)))
        gain = gain * jnp.repeat(heights, shape[axis_at] // shards_of).reshape([-1 if axis == axis_at else 1 for axis in range(len(shape))])
    return gain


def normal_values(key, shape, deviation, bound, cuts=(), held_as=jnp.bfloat16):
    factor_of = block_scale(key, shape, cuts, -0.22, 0.18) if cuts else 1.0
    result = jax.random.normal(key, shape, jnp.float32) * deviation * factor_of
    return jnp.minimum(jnp.maximum(result, -bound), bound).astype(held_as)


def setup_inputs(seed: int = 0) -> dict:
    streams_of = jax.random.split(jax.random.key(seed), 7)
    return {
        "queries": normal_values(streams_of[0], (TOKENS, HEADS * HD), 1.0, 6.0, ((0, 8), (1, 4))),
        "keys": draw_keys(jax.random.fold_in(streams_of[6], 71), 0),
        "values": draw_values(jax.random.fold_in(streams_of[6], 71), 0),
        "gates": jnp.clip(jnp.exp(math.log(1.0) - 2.9957323 * jax.random.uniform(streams_of[3], (TOKENS, HEADS), jnp.float32) ** block_scale(streams_of[3], (TOKENS, HEADS), ((0, 8), (1, 4)), -0.2, 0.2)), 0.05, 1.0),
        "ridge": jnp.clip(jnp.exp(math.log(4.0) - 2.7725887 * jax.random.uniform(streams_of[4], (HEADS,), jnp.float32) ** block_scale(streams_of[4], (HEADS,), ((0, 4),), -0.2, 0.2)), 0.25, 4.0),
        "out_weight": normal_values(streams_of[5], (HEADS * HD, D), (HEADS * HD) ** -0.5, 0.125, ((1, 4),)),
    }


highest = lax.Precision.HIGHEST

def unit_rows(matrix):
    return matrix * lax.rsqrt(lax.optimization_barrier(jnp.sum(matrix * matrix, -1, keepdims=True)) + 1e-06)

def solve_block(prior_gram, prior_moment, keys_unit, keys_gated, values_gated, queries_unit, ridge_column, causal_mask):

    def apply_system(direction):
        from_prior = jnp.einsum('...de,...te->...td', prior_gram, direction, precision=highest)
        correlations = jnp.einsum('...id,...td->...ti', keys_unit, direction, precision=highest) * causal_mask
        from_block = jnp.einsum('...ti,...id->...td', correlations, keys_gated, precision=highest)
        return from_prior + from_block + ridge_column * direction

    def sweep_once(sweep, state):
        solution, residual, direction, norm_now = state
        image = apply_system(direction)
        step_size = norm_now / (lax.optimization_barrier(jnp.sum(direction * image, -1, keepdims=True)) + 1e-06)
        solution = solution + step_size * direction
        residual = residual - step_size * image
        norm_next = lax.optimization_barrier(jnp.sum(residual * residual, -1, keepdims=True))
        direction = residual + norm_next / (norm_now + 1e-06) * direction
        return (solution, residual, direction, norm_next)
    start_state = (jnp.zeros_like(queries_unit), queries_unit, queries_unit, lax.optimization_barrier(jnp.sum(queries_unit * queries_unit, -1, keepdims=True)))
    solution = lax.fori_loop(0, ITERS, sweep_once, start_state)[0]
    correlations = jnp.einsum('...id,...td->...ti', keys_unit, solution, precision=highest) * causal_mask
    readout = jnp.einsum('...ed,...td->...te', prior_moment, solution, precision=highest)
    return readout + jnp.einsum('...ti,...ie->...te', correlations, values_gated, precision=highest)

def reference(queries, keys, values, gates, ridge, out_weight):
    blocks = TOKENS // SPAN

    def split(matrix):
        return matrix.astype(jnp.float32).reshape(blocks, SPAN, HEADS, HD).transpose(0, 2, 1, 3)
    queries_unit = unit_rows(split(queries))
    keys_unit = unit_rows(split(keys))
    gate_cols = gates.astype(jnp.float32).reshape(blocks, SPAN, HEADS).transpose(0, 2, 1)[..., None]
    keys_gated = keys_unit * gate_cols
    values_gated = split(values) * gate_cols
    positions = jnp.arange(SPAN)
    causal_mask = (positions[None, :] <= positions[:, None]).astype(jnp.float32)
    ridge_column = ridge.astype(jnp.float32)[:, None, None]

    def advance(carry, block):
        prior_gram, prior_moment = carry
        unit_block, gated_block, value_block, query_block = block
        readout = solve_block(prior_gram, prior_moment, unit_block, gated_block, value_block, query_block, ridge_column, causal_mask)
        prior_gram = prior_gram + jnp.einsum('hid,hie->hde', gated_block, unit_block, precision=highest)
        prior_moment = prior_moment + jnp.einsum('hie,hid->hed', value_block, unit_block, precision=highest)
        return ((prior_gram, prior_moment), readout)
    zeros = jnp.zeros((HEADS, HD, HD), jnp.float32)
    _, readouts = lax.scan(advance, (zeros, zeros), (keys_unit, keys_gated, values_gated, queries_unit))
    readout = readouts.transpose(0, 2, 1, 3).reshape(TOKENS, HEADS * HD).astype(jnp.bfloat16)
    group_width = HEADS * HD // N_HEAD
    slabs = []
    for group in range(N_HEAD):
        lower = group * group_width
        slabs.append(jnp.dot(readout[:, lower:lower + group_width], out_weight[lower:lower + group_width], preferred_element_type=jnp.float32))
    return jnp.stack(slabs).astype(jnp.bfloat16)
```

```python
import functools

import jax
import jax.numpy as jnp
from jax import lax
from jax.experimental import pallas as pl
from jax.experimental.pallas import tpu as pltpu
from jax.sharding import PartitionSpec as P

HD = 128
SPAN = 128
ITERS = 8
EPS = 1e-06
f32 = jnp.float32
bf16 = jnp.bfloat16
VMEM_BYTES = 56 * 1024 * 1024


def dot(a, b):
    return jnp.dot(a, b, preferred_element_type=f32)


def two_terms(x):
    high = x.astype(bf16)
    return high, (x - high.astype(f32)).astype(bf16)


def inverse_norm(columns):
    return lax.rsqrt(jnp.sum(columns * columns, 0, keepdims=True) + EPS)


def block_sums(keys, values, gate):
    keys_t = keys.astype(f32).T
    s = inverse_norm(keys_t)
    w_value = gate * s
    w_key = w_value * s
    gram = dot(
        jnp.concatenate(two_terms(keys_t * w_key), 1), jnp.concatenate([keys, keys], 0)
    )
    moment = dot(
        jnp.concatenate(two_terms(keys_t * w_value), 1), jnp.concatenate([values, values], 0)
    )
    return gram, moment, keys_t, w_key, w_value


def gate_row(g_ref, h, rows):
    gates = g_ref[:, rows]
    return jnp.sum(
        jnp.where(lax.broadcasted_iota(jnp.int32, gates.shape, 0) == h, gates, 0.0), 0, keepdims=True
    )


def prefix_kernel(
    n_seq, k_ref, v_ref, g_ref, out_ref,
    own, mate, chip_sum, slots, give, final, mate_sems, send_sems, recv_sems, final_sems,
):
    heads = out_ref.shape[0]
    half = heads // 2
    pairs = n_seq // 2
    me = lax.axis_index("seq")
    side = lax.rem(me, 2)
    pair = me // 2
    mate_at = {"seq": me + 1 - 2 * side}
    mine = side * half
    others = (1 - side) * half

    barrier = pltpu.get_barrier_semaphore()
    pl.semaphore_signal(barrier, inc=1, device_id=mate_at, device_id_type=pl.DeviceIdType.MESH)
    for off in range(1, pairs):
        target = {"seq": lax.rem(pair + off, pairs) * 2 + side}
        pl.semaphore_signal(barrier, inc=1, device_id=target, device_id_type=pl.DeviceIdType.MESH)

    def sum_head(h):
        gram = jnp.zeros((HD, HD), f32)
        moment = jnp.zeros((HD, HD), f32)
        columns = pl.ds(pl.multiple_of(h * HD, HD), HD)
        for c in range(k_ref.shape[0] // SPAN):
            rows = pl.ds(c * SPAN, SPAN)
            block_gram, block_moment, *_ = block_sums(
                k_ref[rows, columns], v_ref[rows, columns], gate_row(g_ref, h, rows)
            )
            gram += block_gram
            moment += block_moment
        own[h, 0] = gram
        own[h, 1] = moment

    for j in range(half):
        sum_head(others + j)
    pl.semaphore_wait(barrier, pairs)
    to_mate = pltpu.make_async_remote_copy(
        src_ref=own.at[pl.ds(others, half)], dst_ref=mate,
        send_sem=mate_sems.at[0], recv_sem=mate_sems.at[1],
        device_id=mate_at, device_id_type=pl.DeviceIdType.MESH,
    )
    to_mate.start()
    for j in range(half):
        sum_head(mine + j)
    to_mate.wait()
    chip_sum[...] = own[pl.ds(mine, half)] + mate[...]

    def to_later(off):
        target = {"seq": lax.rem(pair + off, pairs) * 2 + side}
        return pltpu.make_async_remote_copy(
            src_ref=chip_sum, dst_ref=slots.at[off - 1],
            send_sem=send_sems.at[off - 1], recv_sem=recv_sems.at[off - 1],
            device_id=target, device_id_type=pl.DeviceIdType.MESH,
        )

    for off in range(1, pairs):
        @pl.when(pair + off < pairs)
        def _():
            to_later(off).start()

    give[...] = jnp.zeros(give.shape, f32)
    for off in range(1, pairs):
        @pl.when(pair >= off)
        def _():
            to_later(off).wait_recv()
            give[...] = give[...] + slots[off - 1]

    out_ref[pl.ds(mine, half)] = give[...] + side.astype(f32) * mate[...]
    give[...] = give[...] + (1 - side).astype(f32) * own[pl.ds(mine, half)]
    back = pltpu.make_async_remote_copy(
        src_ref=give, dst_ref=final,
        send_sem=final_sems.at[0], recv_sem=final_sems.at[1],
        device_id=mate_at, device_id_type=pl.DeviceIdType.MESH,
    )
    back.start()
    back.wait()
    out_ref[pl.ds(others, half)] = final[...]
    for off in range(1, pairs):
        @pl.when(pair + off < pairs)
        def _():
            to_later(off).wait_send()


def row_sum(x):
    return jnp.sum(x, 1, keepdims=True)


def solve_kernel(
    q_ref, k_ref, v_ref, g_ref, ridge_ref, prior_ref, out_ref,
    gram_high, gram_low, keys_t, keys_w, values_w, moment_high, moment_low, sol, res, direct, norms,
):
    h = pl.program_id(0)
    blocks = k_ref.shape[0] // SPAN
    row = lax.broadcasted_iota(jnp.int32, (HD, HD), 0)
    col = lax.broadcasted_iota(jnp.int32, (HD, HD), 1)
    causal = (col <= row).astype(f32).astype(bf16)
    total = jnp.concatenate([jnp.where(row == col, ridge_ref[h], 0.0) + prior_ref[0], prior_ref[1]], 1)
    for c in range(blocks):
        rows = pl.ds(c * SPAN, SPAN)
        keys = k_ref[rows]
        keys_f = keys.astype(f32)
        s = lax.rsqrt(row_sum(keys_f * keys_f) + EPS)
        gates = g_ref[rows, :]
        gate = row_sum(jnp.where(lax.broadcasted_iota(jnp.int32, gates.shape, 1) == h, gates, 0.0))
        w_value = gate * s
        both = jnp.concatenate([keys_f * (w_value * s), v_ref[rows].astype(f32) * w_value], 1)
        high, low = two_terms(both)
        turned = keys.T
        keys_t[c] = turned
        keys_w[c] = high[:, :HD]
        values_w[c] = high[:, HD:]
        total_high, total_low = two_terms(total)
        gram_high[c] = total_high[:, :HD]
        gram_low[c] = total_low[:, :HD]
        moment_high[c] = total_high[:, HD:]
        moment_low[c] = total_low[:, HD:]
        total += dot(jnp.concatenate([turned, turned], 1), jnp.concatenate([high, low], 0))
        queries = q_ref[rows].astype(f32)
        queries = queries * lax.rsqrt(row_sum(queries * queries) + EPS)
        res[c] = queries
        direct[c] = queries
        sol[c] = jnp.zeros((SPAN, HD), f32)
        norms[c] = jnp.broadcast_to(row_sum(queries * queries), (SPAN, HD))

    def apply(c, d, high_ref, low_ref, right_ref):
        high, low = two_terms(d)
        half = jnp.concatenate([high_ref[c], keys_t[c]], 1)
        first = dot(jnp.concatenate([high, low], 1), jnp.concatenate([half, half], 0))
        corr = first[:, HD:].astype(bf16) * causal
        return first[:, :HD] + dot(
            jnp.concatenate([corr, high], 1), jnp.concatenate([right_ref[c], low_ref[c]], 0)
        )

    def sweep(_, carry):
        for c in range(blocks):
            d = direct[c]
            image = apply(c, d, gram_high, gram_low, keys_w)
            now = norms[c]
            step = now / (row_sum(d * image) + EPS)
            sol[c] = sol[c] + step * d
            r = res[c] - step * image
            res[c] = r
            following = jnp.broadcast_to(row_sum(r * r), (SPAN, HD))
            norms[c] = following
            direct[c] = r + following / (now + EPS) * d
        return carry

    lax.fori_loop(0, ITERS, sweep, 0)
    for c in range(blocks):
        out_ref[pl.ds(c * SPAN, SPAN)] = apply(
            c, sol[c], moment_high, moment_low, values_w
        ).astype(out_ref.dtype)


def project_kernel(r_ref, *refs):
    *pieces, out_ref = refs
    count = len(pieces)
    me = lax.axis_index("head")
    readout = r_ref[...]
    for shift, piece in enumerate(pieces):
        width = piece.shape[1]
        owner = lax.rem(me + count - shift, count)
        columns = pl.ds(pl.multiple_of(owner * width, width), width)
        out_ref[0, :, columns] = dot(readout, piece[...]).astype(out_ref.dtype)


def shards(n_seq, n_head, queries, keys, values, gates, ridge, out_weight):
    tokens, head_width = queries.shape
    heads = head_width // HD
    blocks = tokens // SPAN
    me = lax.axis_index("head")

    def rows_of(device):
        return lax.dynamic_slice_in_dim(out_weight, device * head_width, head_width, 0)

    pieces = [rows_of(me)]
    for shift in range(1, n_head):
        pairs = [(i, (i + shift) % n_head) for i in range(n_head)]
        pieces.append(lax.ppermute(rows_of(lax.rem(me + shift, n_head)), "head", pairs))

    gate_rows = gates.T
    by_head = pl.BlockSpec((tokens, HD), lambda h: (0, h))
    gate_spec = pl.BlockSpec((heads, tokens), lambda h: (0, 0))
    params = pltpu.CompilerParams(vmem_limit_bytes=VMEM_BYTES)
    tile = SPAN * HD * HD * 2
    half = heads // 2
    pairs = n_seq // 2
    part = pltpu.VMEM((half, 2, HD, HD), f32)
    in_vmem = pl.BlockSpec(memory_space=pltpu.VMEM)
    prior = pl.pallas_call(
        functools.partial(prefix_kernel, n_seq),
        in_specs=[in_vmem] * 3,
        out_specs=in_vmem,
        out_shape=jax.ShapeDtypeStruct((heads, 2, HD, HD), f32),
        scratch_shapes=[
            pltpu.VMEM((heads, 2, HD, HD), f32),
            part, part,
            pltpu.VMEM((pairs - 1, half, 2, HD, HD), f32),
            part, part,
            pltpu.SemaphoreType.DMA((2,)),
            pltpu.SemaphoreType.DMA((pairs - 1,)),
            pltpu.SemaphoreType.DMA((pairs - 1,)),
            pltpu.SemaphoreType.DMA((2,)),
        ],
        compiler_params=pltpu.CompilerParams(
            vmem_limit_bytes=VMEM_BYTES, collective_id=0, has_side_effects=True
        ),
        cost_estimate=pl.CostEstimate(
            flops=heads * blocks * 4 * tile, bytes_accessed=tokens * head_width * 4, transcendentals=0
        ),
        name="prefix",
    )(keys, values, gate_rows)
    state = pltpu.VMEM((blocks, HD, SPAN), f32)
    tile_bf16 = pltpu.VMEM((blocks, SPAN, HD), bf16)
    readout = pl.pallas_call(
        solve_kernel,
        grid=(heads,),
        in_specs=[
            by_head, by_head, by_head, pl.BlockSpec((tokens, heads), lambda h: (0, 0)),
            pl.BlockSpec(memory_space=pltpu.SMEM),
            pl.BlockSpec((None, 2, HD, HD), lambda h: (h, 0, 0, 0)),
        ],
        out_specs=by_head,
        out_shape=jax.ShapeDtypeStruct((tokens, head_width), bf16),
        scratch_shapes=[
            *[tile_bf16] * 7,
            state, state, state, state,
        ],
        compiler_params=params,
        cost_estimate=pl.CostEstimate(
            flops=heads * blocks * 54 * tile, bytes_accessed=tokens * head_width * 8, transcendentals=0
        ),
        name="solve",
    )(queries, keys, values, gates, ridge, prior)
    width = out_weight.shape[1]
    rows = 2 * SPAN
    whole = pl.BlockSpec((head_width, width), lambda i: (0, 0))
    return pl.pallas_call(
        project_kernel,
        grid=(tokens // rows,),
        in_specs=[pl.BlockSpec((rows, head_width), lambda i: (i, 0))] + [whole] * n_head,
        out_specs=pl.BlockSpec((1, rows, width * n_head), lambda i: (0, i, 0)),
        out_shape=jax.ShapeDtypeStruct((1, tokens, width * n_head), bf16),
        compiler_params=params,
        cost_estimate=pl.CostEstimate(
            flops=2 * tokens * head_width * width * n_head,
            bytes_accessed=tokens * width * n_head * 2,
            transcendentals=0,
        ),
        name="project",
    )(readout, *pieces)


def solution(mesh):
    return jax.shard_map(
        functools.partial(shards, mesh.shape["seq"], mesh.shape["head"]),
        mesh=mesh,
        in_specs=(
            P("seq", "head"),
            P("seq", "head"),
            P("seq", "head"),
            P("seq", "head"),
            P("head"),
            P(None, "head"),
        ),
        out_specs=P("head", "seq", None),
        check_vma=False,
    )
```

```python
import functools

import jax
import jax.numpy as jnp
from jax import lax
from jax.experimental import pallas as pl
from jax.experimental.pallas import tpu as pltpu
from jax.sharding import PartitionSpec as P

HD = 128
SPAN = 128
ITERS = 8
EPS = 1e-06
f32 = jnp.float32
bf16 = jnp.bfloat16
VMEM_BYTES = 56 * 1024 * 1024
MESH = pl.DeviceIdType.MESH


def dot(a, b):
    return jnp.dot(a, b, preferred_element_type=f32)


def two_terms(x):
    high = x.astype(bf16)
    return high, (x - high.astype(f32)).astype(bf16)


def row_sum(x):
    return jnp.sum(x, 1, keepdims=True)


def wide(x):
    return jnp.broadcast_to(x, (SPAN, HD))


def solve_kernel(
    n_seq, n_head,
    k_hbm, v_hbm, q_hbm, g_ref, ridge_ref, w_hbm, out_ref, pieces_ref,
    k_ref, v_ref, q_ref, keys_t, keys_w, values_w, scales, gram_local, moment_local,
    gram_high, gram_low, direct, res, sol, norms, images,
    own, mate, chip_sum, slots, give, prior,
    load_sems, piece_sems, mate_sems, send_sems, recv_sems, back_sems,
):
    tokens, head_width = k_ref.shape
    heads = head_width // HD
    half = heads // 2
    blocks = tokens // SPAN
    pairs = n_seq // 2
    me = lax.axis_index("seq")
    group = lax.axis_index("head")
    side = lax.rem(me, 2)
    pair = me // 2
    mate_at = {"seq": me + 1 - 2 * side}
    mine = side * half
    others = (1 - side) * half
    row = lax.broadcasted_iota(jnp.int32, (HD, HD), 0)
    col = lax.broadcasted_iota(jnp.int32, (HD, HD), 1)
    causal = (col <= row).astype(f32).astype(bf16)
    GRAM, MOMENT = 0, 1

    loads = [
        pltpu.make_async_copy(src, dst, load_sems.at[i])
        for i, (src, dst) in enumerate(((k_hbm, k_ref), (v_hbm, v_ref), (q_hbm, q_ref)))
    ]
    for load in loads:
        load.start()

    barrier = pltpu.get_barrier_semaphore()
    pl.semaphore_signal(barrier, inc=1, device_id=mate_at, device_id_type=MESH)
    for off in range(1, pairs):
        target = {"seq": lax.rem(pair + off, pairs) * 2 + side}
        pl.semaphore_signal(barrier, inc=1, device_id=target, device_id_type=MESH)
    for shift in range(1, n_head):
        target = {"head": lax.rem(group + shift, n_head)}
        pl.semaphore_signal(barrier, inc=1, device_id=target, device_id_type=MESH)

    def columns_of(h):
        return pl.ds(pl.multiple_of(h * HD, HD), HD)

    def sum_grams(first):
        def one(j, carry):
            h = first + j
            total = jnp.zeros((HD, HD), f32)
            for c in range(blocks):
                n = h * blocks + c
                rows = pl.ds(c * SPAN, SPAN)
                keys = k_ref[rows, columns_of(h)]
                keys_f = keys.astype(f32)
                s = lax.rsqrt(row_sum(keys_f * keys_f) + EPS)
                gates = g_ref[rows, :]
                gate = row_sum(jnp.where(lax.broadcasted_iota(jnp.int32, gates.shape, 1) == h, gates, 0.0))
                w_value = gate * s
                high, low = two_terms(keys_f * (w_value * s))
                turned = keys.T
                keys_t[n] = turned
                keys_w[n] = high
                scales[n] = wide(w_value)
                gram_local[n] = total
                total += dot(jnp.concatenate([turned, turned], 1), jnp.concatenate([high, low], 0))
            own[GRAM, h] = total
            return carry

        lax.fori_loop(0, half, one, 0)

    def sum_moments(first):
        def one(j, carry):
            h = first + j
            total = jnp.zeros((HD, HD), f32)
            for c in range(blocks):
                n = h * blocks + c
                values = v_ref[pl.ds(c * SPAN, SPAN), columns_of(h)].astype(f32)
                high, low = two_terms(values * scales[n])
                values_w[n] = high
                moment_local[n] = total
                turned = keys_t[n]
                total += dot(jnp.concatenate([turned, turned], 1), jnp.concatenate([high, low], 0))
            own[MOMENT, h] = total
            return carry

        lax.fori_loop(0, half, one, 0)

    def to_mate(kind):
        return pltpu.make_async_remote_copy(
            src_ref=own.at[kind, pl.ds(others, half)], dst_ref=mate.at[kind],
            send_sem=mate_sems.at[kind, 0], recv_sem=mate_sems.at[kind, 1],
            device_id=mate_at, device_id_type=MESH,
        )

    def to_later(kind, off):
        target = {"seq": lax.rem(pair + off, pairs) * 2 + side}
        return pltpu.make_async_remote_copy(
            src_ref=chip_sum.at[kind], dst_ref=slots.at[kind, off - 1],
            send_sem=send_sems.at[kind, off - 1], recv_sem=recv_sems.at[kind, off - 1],
            device_id=target, device_id_type=MESH,
        )

    def to_back(kind):
        return pltpu.make_async_remote_copy(
            src_ref=give.at[kind], dst_ref=prior.at[kind, 1],
            send_sem=back_sems.at[kind, 0], recv_sem=back_sems.at[kind, 1],
            device_id=mate_at, device_id_type=MESH,
        )

    def to_head(shift):
        target = lax.rem(group + shift, n_head)
        return pltpu.make_async_remote_copy(
            src_ref=w_hbm.at[pl.ds(pl.multiple_of(target * head_width, head_width), head_width)],
            dst_ref=pieces_ref.at[shift - 1],
            send_sem=piece_sems.at[0, shift - 1], recv_sem=piece_sems.at[1, shift - 1],
            device_id={"head": target}, device_id_type=MESH,
        )

    def pass_on(kind):
        to_mate(kind).wait_recv()
        chip_sum[kind] = own[kind, pl.ds(mine, half)] + mate[kind]
        for off in range(1, pairs):
            @pl.when(pair + off < pairs)
            def _():
                to_later(kind, off).start()

    def collect(kind):
        total = jnp.zeros((half, HD, HD), f32)
        give[kind] = total
        for off in range(1, pairs):
            @pl.when(pair >= off)
            def _():
                to_later(kind, off).wait_recv()
                give[kind] = give[kind] + slots[kind, off - 1]
        prior[kind, 0] = give[kind] + side.astype(f32) * mate[kind]
        give[kind] = give[kind] + (1 - side).astype(f32) * own[kind, pl.ds(mine, half)]
        to_back(kind).start()

    loads[0].wait()
    sum_grams(others)
    pl.semaphore_wait(barrier, pairs + n_head - 1)
    to_mate(GRAM).start()
    for shift in range(1, n_head):
        to_head(shift).start()
    sum_grams(mine)
    pass_on(GRAM)
    loads[1].wait()
    sum_moments(others)
    to_mate(MOMENT).start()
    sum_moments(mine)
    pass_on(MOMENT)
    loads[2].wait()
    collect(GRAM)

    def apply(n, at, d, high_ref, low_ref, right_ref, fine=True):
        half_right = jnp.concatenate([high_ref[n], keys_t[at]], 1)
        if fine:
            high, low = two_terms(d)
            first = dot(jnp.concatenate([high, low], 1), jnp.concatenate([half_right, half_right], 0))
        else:
            high = d.astype(bf16)
            first = dot(high, half_right)
        corr = first[:, HD:].astype(bf16) * causal
        if fine:
            left = jnp.concatenate([corr, high], 1)
            right = jnp.concatenate([right_ref[at], low_ref[n]], 0)
        else:
            left, right = corr, right_ref[at]
        second = dot(left, jnp.concatenate([right, right], 1))
        return first[:, :HD] + second[:, :HD]

    units = half * blocks
    behind = units // 2

    def run(p, carry):
        first = mine + p * (others - mine)

        @pl.when(p == 1)
        def _():
            to_back(GRAM).wait_recv()

        def split(kind, j, c, local, low_too=None):
            total = local[(first + j) * blocks + c] + prior[kind, p, j]
            if kind == GRAM:
                total += jnp.where(row == col, ridge_ref[first + j], 0.0)
            gram_high[j * blocks + c], gram_low[j * blocks + c] = two_terms(total)

        def prepare(j, carry):
            for c in range(blocks):
                n = j * blocks + c
                split(GRAM, j, c, gram_local)
                queries = q_ref[pl.ds(c * SPAN, SPAN), columns_of(first + j)].astype(f32)
                square = row_sum(queries * queries)
                scale = lax.rsqrt(square + EPS)
                queries = queries * scale
                res[n] = queries
                direct[n] = queries
                sol[n] = jnp.zeros((SPAN, HD), f32)
                norms[n] = wide(square * scale * scale)
            return carry

        lax.fori_loop(0, half, prepare, 0)

        def multiply(n, fine=True):
            images[n] = apply(n, first * blocks + n, direct[n], gram_high, gram_low, keys_w, fine)

        def update(n, last=False):
            d = direct[n]
            image = images[n]
            now = norms[n]
            step = now / (row_sum(d * image) + EPS)
            sol[n] = sol[n] + step * d
            if last:
                return
            r = res[n] - step * image
            res[n] = r
            following = wide(row_sum(r * r))
            norms[n] = following
            direct[n] = r + following / (now + EPS) * d

        def iteration(last=False, before_last=False):
            for n in range(behind):
                multiply(n, not last)
                update(behind + n, last)
            for n in range(behind):
                update(n, last)
                if not last:
                    multiply(behind + n, not before_last)

        for n in range(behind):
            multiply(behind + n)

        def sweep(_, carry):
            iteration()
            iteration()
            return carry

        lax.fori_loop(0, (ITERS - 2) // 2, sweep, 0)
        iteration(before_last=True)
        iteration(last=True)

        @pl.when(p == 0)
        def _():
            collect(MOMENT)

        @pl.when(p == 1)
        def _():
            to_back(MOMENT).wait_recv()

        def finish(j, carry):
            for c in range(blocks):
                split(MOMENT, j, c, moment_local)
            for c in range(blocks):
                n = j * blocks + c
                out_ref[pl.ds(c * SPAN, SPAN), columns_of(first + j)] = apply(
                    n, first * blocks + n, sol[n], gram_high, gram_low, values_w
                ).astype(out_ref.dtype)
            return carry

        lax.fori_loop(0, half, finish, 0)
        return carry

    lax.fori_loop(0, 2, run, 0)
    for kind in (GRAM, MOMENT):
        to_mate(kind).wait_send()
        to_back(kind).wait_send()
        for off in range(1, pairs):
            @pl.when(pair + off < pairs)
            def _():
                to_later(kind, off).wait_send()
    for shift in range(1, n_head):
        to_head(shift).wait()


def project_kernel(r_ref, w_hbm, pieces_ref, out_ref, weight, sems):
    count = pieces_ref.shape[0] + 1
    depth, width = pieces_ref.shape[1:]
    me = lax.axis_index("head")

    @pl.when(pl.program_id(0) == 0)
    def _():
        copies = []
        for shift in range(count):
            owner = lax.rem(me + count - shift, count)
            if shift:
                source = pieces_ref.at[shift - 1]
            else:
                source = w_hbm.at[pl.ds(pl.multiple_of(me * depth, depth), depth)]
            columns = pl.ds(pl.multiple_of(owner * width, width), width)
            copies.append(pltpu.make_async_copy(source, weight.at[:, columns], sems.at[shift]))
        for copy in copies:
            copy.start()
        for copy in copies:
            copy.wait()

    out_ref[0] = dot(r_ref[...], weight[...]).astype(out_ref.dtype)


def shards(n_seq, n_head, queries, keys, values, gates, ridge, out_weight):
    tokens, head_width = queries.shape
    heads = head_width // HD
    half = heads // 2
    blocks = tokens // SPAN
    pairs = n_seq // 2
    width = out_weight.shape[1]
    tile = SPAN * HD * HD * 2
    hbm = pl.BlockSpec(memory_space=pl.ANY)
    in_vmem = pl.BlockSpec(memory_space=pltpu.VMEM)

    def square(*lead, dtype=f32):
        return pltpu.VMEM((*lead, HD, HD), dtype)

    every, some = heads * blocks, half * blocks
    readout, pieces = pl.pallas_call(
        functools.partial(solve_kernel, n_seq, n_head),
        in_specs=[hbm, hbm, hbm, in_vmem, pl.BlockSpec(memory_space=pltpu.SMEM), hbm],
        out_specs=[in_vmem, hbm],
        out_shape=[
            jax.ShapeDtypeStruct((tokens, head_width), bf16),
            jax.ShapeDtypeStruct((n_head - 1, head_width, width), bf16),
        ],
        scratch_shapes=[
            *[pltpu.VMEM((tokens, head_width), bf16)] * 3,
            *[square(every, dtype=bf16)] * 3,
            *[square(every)] * 3,
            *[square(some, dtype=bf16)] * 2,
            *[square(some)] * 5,
            square(2, heads),
            square(2, half), square(2, half), square(2, pairs - 1, half), square(2, half), square(2, 2, half),
            pltpu.SemaphoreType.DMA((3,)),
            pltpu.SemaphoreType.DMA((2, n_head - 1)),
            pltpu.SemaphoreType.DMA((2, 2)),
            pltpu.SemaphoreType.DMA((2, pairs - 1)),
            pltpu.SemaphoreType.DMA((2, pairs - 1)),
            pltpu.SemaphoreType.DMA((2, 2)),
        ],
        compiler_params=pltpu.CompilerParams(
            vmem_limit_bytes=VMEM_BYTES, collective_id=0, has_side_effects=True
        ),
        cost_estimate=pl.CostEstimate(
            flops=heads * blocks * 58 * tile, bytes_accessed=tokens * head_width * 8, transcendentals=0
        ),
        name="solve",
    )(keys, values, queries, gates, ridge, out_weight)
    rows = 2 * SPAN
    return pl.pallas_call(
        project_kernel,
        grid=(tokens // rows,),
        in_specs=[pl.BlockSpec((rows, head_width), lambda i: (i, 0)), hbm, hbm],
        out_specs=pl.BlockSpec((1, rows, width * n_head), lambda i: (0, i, 0)),
        out_shape=jax.ShapeDtypeStruct((1, tokens, width * n_head), bf16),
        scratch_shapes=[
            pltpu.VMEM((head_width, width * n_head), bf16),
            pltpu.SemaphoreType.DMA((n_head,)),
        ],
        compiler_params=pltpu.CompilerParams(vmem_limit_bytes=VMEM_BYTES),
        cost_estimate=pl.CostEstimate(
            flops=2 * tokens * head_width * width * n_head,
            bytes_accessed=tokens * width * n_head * 2,
            transcendentals=0,
        ),
        name="project",
    )(readout, out_weight, pieces)


def solution(mesh):
    return jax.shard_map(
        functools.partial(shards, mesh.shape["seq"], mesh.shape["head"]),
        mesh=mesh,
        in_specs=(
            P("seq", "head"),
            P("seq", "head"),
            P("seq", "head"),
            P("seq", "head"),
            P("head"),
            P(None, "head"),
        ),
        out_specs=P("head", "seq", None),
        check_vma=False,
    )
```

```python
import functools

import jax
import jax.numpy as jnp
from jax import lax
from jax.experimental import pallas as pl
from jax.experimental.pallas import tpu as pltpu
from jax.sharding import PartitionSpec as P

HD = 128
SPAN = 128
ITERS = 8
EPS = 1e-06
f32 = jnp.float32
bf16 = jnp.bfloat16
VMEM_BYTES = 56 * 1024 * 1024
MESH = pl.DeviceIdType.MESH


def dot(a, b):
    return jnp.dot(a, b, preferred_element_type=f32)


def two_terms(x):
    high = x.astype(bf16)
    return high, (x - high.astype(f32)).astype(bf16)


def row_sum(x):
    return jnp.sum(x, 1, keepdims=True)


def wide(x):
    return jnp.broadcast_to(x, (SPAN, HD))


def solve_kernel(
    n_seq, n_head,
    k_hbm, v_hbm, q_hbm, g_ref, ridge_ref, w_hbm, out_ref, pieces_ref,
    k_ref, v_ref, q_ref, gate_columns, keys_t, keys_w, values_w, scales, gram_local, moment_local,
    gram_high, gram_low, direct, res, sol, norms, images,
    own, mate, chip_sum, slots, give, prior,
    load_sems, piece_sems, plane_sems, chip_sems, mate_sems, send_sems, recv_sems, back_sems,
):
    tokens, head_width = k_ref.shape
    heads = head_width // HD
    half = heads // 2
    blocks = tokens // SPAN
    pairs = n_seq // 2
    me = lax.axis_index("seq")
    group = lax.axis_index("head")
    side = lax.rem(me, 2)
    pair = me // 2
    mate_at = {"seq": me + 1 - 2 * side}
    mine = side * half
    others = (1 - side) * half
    row = lax.broadcasted_iota(jnp.int32, (HD, HD), 0)
    col = lax.broadcasted_iota(jnp.int32, (HD, HD), 1)
    causal = (col <= row).astype(f32).astype(bf16)
    GRAM, MOMENT = 0, 1

    loads = [
        pltpu.make_async_copy(src, dst, load_sems.at[i])
        for i, (src, dst) in enumerate(((k_hbm, k_ref), (v_hbm, v_ref), (q_hbm, q_ref)))
    ]
    for load in loads:
        load.start()

    barrier = pltpu.get_barrier_semaphore()
    pl.semaphore_signal(barrier, inc=1, device_id=mate_at, device_id_type=MESH)
    for off in range(1, pairs):
        target = {"seq": lax.rem(pair + off, pairs) * 2 + side}
        pl.semaphore_signal(barrier, inc=1, device_id=target, device_id_type=MESH)
    for shift in range(1, n_head):
        target = {"head": lax.rem(group + shift, n_head)}
        pl.semaphore_signal(barrier, inc=1, device_id=target, device_id_type=MESH)

    for c in range(blocks):
        rows = pl.ds(c * SPAN, SPAN)
        gate_columns[rows, :] = g_ref[:, rows].T

    def columns_of(h):
        return pl.ds(pl.multiple_of(h * HD, HD), HD)

    def sum_grams(first):
        def one(j, carry):
            h = first + j
            total = jnp.zeros((HD, HD), f32)
            for c in range(blocks):
                n = h * blocks + c
                rows = pl.ds(c * SPAN, SPAN)
                keys = k_ref[rows, columns_of(h)]
                keys_f = keys.astype(f32)
                s = lax.rsqrt(row_sum(keys_f * keys_f) + EPS)
                gates = gate_columns[rows, :]
                gate = row_sum(jnp.where(lax.broadcasted_iota(jnp.int32, gates.shape, 1) == h, gates, 0.0))
                w_value = gate * s
                high, low = two_terms(keys_f * (w_value * s))
                turned = keys.T
                keys_t[n] = turned
                keys_w[n] = high
                scales[n] = wide(w_value)
                gram_local[n] = total
                total += dot(jnp.concatenate([turned, turned], 1), jnp.concatenate([high, low], 0))
            own[GRAM, h] = total
            return carry

        lax.fori_loop(0, half, one, 0)

    def sum_moments(first):
        def one(j, carry):
            h = first + j
            total = jnp.zeros((HD, HD), f32)
            for c in range(blocks):
                n = h * blocks + c
                values = v_ref[pl.ds(c * SPAN, SPAN), columns_of(h)].astype(f32)
                high, low = two_terms(values * scales[n])
                values_w[n] = high
                moment_local[n] = total
                turned = keys_t[n]
                total += dot(jnp.concatenate([turned, turned], 1), jnp.concatenate([high, low], 0))
            own[MOMENT, h] = total
            return carry

        lax.fori_loop(0, half, one, 0)

    def to_mate(kind):
        return pltpu.make_async_remote_copy(
            src_ref=own.at[kind, pl.ds(others, half)], dst_ref=mate.at[kind],
            send_sem=mate_sems.at[kind, 0], recv_sem=mate_sems.at[kind, 1],
            device_id=mate_at, device_id_type=MESH,
        )

    def to_later(kind, off):
        target = {"seq": lax.rem(pair + off, pairs) * 2 + side}
        return pltpu.make_async_remote_copy(
            src_ref=chip_sum.at[kind], dst_ref=slots.at[kind, off - 1],
            send_sem=send_sems.at[kind, off - 1], recv_sem=recv_sems.at[kind, off - 1],
            device_id=target, device_id_type=MESH,
        )

    def to_back(kind):
        return pltpu.make_async_remote_copy(
            src_ref=give.at[kind], dst_ref=prior.at[kind, 1],
            send_sem=back_sems.at[kind, 0], recv_sem=back_sems.at[kind, 1],
            device_id=mate_at, device_id_type=MESH,
        )

    part = head_width // n_seq

    def to_head(shift):
        target = lax.rem(group + shift, n_head)
        start = pl.multiple_of(target * head_width + me * part, part)
        return pltpu.make_async_remote_copy(
            src_ref=w_hbm.at[pl.ds(start, part)], dst_ref=pieces_ref.at[shift - 1, pair, side],
            send_sem=piece_sems.at[0, shift - 1], recv_sem=piece_sems.at[1, shift - 1],
            device_id={"head": target}, device_id_type=MESH,
        )

    def to_plane(off):
        mine_part = pieces_ref.at[:, pair, side]
        target = {"seq": lax.rem(pair + off, pairs) * 2 + side}
        return pltpu.make_async_remote_copy(
            src_ref=mine_part, dst_ref=mine_part,
            send_sem=plane_sems.at[0, off - 1], recv_sem=plane_sems.at[1, off - 1],
            device_id=target, device_id_type=MESH,
        )

    def to_chip():
        mine_parts = pieces_ref.at[:, :, side]
        return pltpu.make_async_remote_copy(
            src_ref=mine_parts, dst_ref=mine_parts,
            send_sem=chip_sems.at[0], recv_sem=chip_sems.at[1],
            device_id=mate_at, device_id_type=MESH,
        )

    def pass_on(kind):
        to_mate(kind).wait_recv()
        chip_sum[kind] = own[kind, pl.ds(mine, half)] + mate[kind]
        for off in range(1, pairs):
            @pl.when(pair + off < pairs)
            def _():
                to_later(kind, off).start()

    def collect(kind):
        total = jnp.zeros((half, HD, HD), f32)
        give[kind] = total
        for off in range(1, pairs):
            @pl.when(pair >= off)
            def _():
                to_later(kind, off).wait_recv()
                give[kind] = give[kind] + slots[kind, off - 1]
        prior[kind, 0] = give[kind] + side.astype(f32) * mate[kind]
        give[kind] = give[kind] + (1 - side).astype(f32) * own[kind, pl.ds(mine, half)]
        to_back(kind).start()

    loads[0].wait()
    sum_grams(others)
    pl.semaphore_wait(barrier, pairs + n_head - 1)
    to_mate(GRAM).start()
    for shift in range(1, n_head):
        to_head(shift).start()
    sum_grams(mine)
    pass_on(GRAM)
    loads[1].wait()
    sum_moments(others)
    to_mate(MOMENT).start()
    sum_moments(mine)
    pass_on(MOMENT)
    loads[2].wait()
    collect(GRAM)
    for shift in range(1, n_head):
        to_head(shift).wait_recv()
    for off in range(1, pairs):
        to_plane(off).start()

    def apply(n, at, d, high_ref, low_ref, right_ref, fine=True):
        half_right = jnp.concatenate([high_ref[n], keys_t[at]], 1)
        if fine:
            high, low = two_terms(d)
            first = dot(jnp.concatenate([high, low], 1), jnp.concatenate([half_right, half_right], 0))
        else:
            high = d.astype(bf16)
            first = dot(high, half_right)
        corr = first[:, HD:].astype(bf16) * causal
        if fine:
            left = jnp.concatenate([corr, high], 1)
            right = jnp.concatenate([right_ref[at], low_ref[n]], 0)
        else:
            left, right = corr, right_ref[at]
        second = dot(left, jnp.concatenate([right, right], 1))
        return first[:, :HD] + second[:, :HD]

    units = half * blocks
    behind = units // 2

    def run(p, carry):
        first = mine + p * (others - mine)

        @pl.when(p == 1)
        def _():
            to_back(GRAM).wait_recv()

        def split(kind, j, c, local, low_too=None):
            total = local[(first + j) * blocks + c] + prior[kind, p, j]
            if kind == GRAM:
                total += jnp.where(row == col, ridge_ref[first + j], 0.0)
            gram_high[j * blocks + c], gram_low[j * blocks + c] = two_terms(total)

        def prepare(j, carry):
            for c in range(blocks):
                n = j * blocks + c
                split(GRAM, j, c, gram_local)
                queries = q_ref[pl.ds(c * SPAN, SPAN), columns_of(first + j)].astype(f32)
                square = row_sum(queries * queries)
                scale = lax.rsqrt(square + EPS)
                queries = queries * scale
                res[n] = queries
                direct[n] = queries
                sol[n] = jnp.zeros((SPAN, HD), f32)
                norms[n] = wide(square * scale * scale)
            return carry

        lax.fori_loop(0, half, prepare, 0)

        def multiply(n, fine=True):
            images[n] = apply(n, first * blocks + n, direct[n], gram_high, gram_low, keys_w, fine)

        def update(n, last=False):
            d = direct[n]
            image = images[n]
            now = norms[n]
            step = now / (row_sum(d * image) + EPS)
            sol[n] = sol[n] + step * d
            if last:
                return
            r = res[n] - step * image
            res[n] = r
            following = wide(row_sum(r * r))
            norms[n] = following
            direct[n] = r + following / (now + EPS) * d

        def iteration(last=False, before_last=False):
            for n in range(behind):
                multiply(n, not last)
                update(behind + n, last)
            for n in range(behind):
                update(n, last)
                if not last:
                    multiply(behind + n, not before_last)

        for n in range(behind):
            multiply(behind + n)

        def sweep(_, carry):
            iteration()
            iteration()
            return carry

        lax.fori_loop(0, (ITERS - 2) // 2, sweep, 0)
        iteration(before_last=True)
        iteration(last=True)

        @pl.when(p == 0)
        def _():
            collect(MOMENT)
            for off in range(1, pairs):
                to_plane(off).wait_recv()
            to_chip().start()

        @pl.when(p == 1)
        def _():
            to_back(MOMENT).wait_recv()

        def finish(j, carry):
            for c in range(blocks):
                split(MOMENT, j, c, moment_local)
            for c in range(blocks):
                n = j * blocks + c
                out_ref[pl.ds(c * SPAN, SPAN), columns_of(first + j)] = apply(
                    n, first * blocks + n, sol[n], gram_high, gram_low, values_w
                ).astype(out_ref.dtype)
            return carry

        lax.fori_loop(0, half, finish, 0)
        return carry

    lax.fori_loop(0, 2, run, 0)
    for kind in (GRAM, MOMENT):
        to_mate(kind).wait_send()
        to_back(kind).wait_send()
        for off in range(1, pairs):
            @pl.when(pair + off < pairs)
            def _():
                to_later(kind, off).wait_send()
    for shift in range(1, n_head):
        to_head(shift).wait_send()
    for off in range(1, pairs):
        to_plane(off).wait_send()
    to_chip().wait()


def project_kernel(r_ref, w_hbm, pieces_ref, out_ref, weight, sems):
    count = pieces_ref.shape[0] + 1
    depth, width = pieces_ref.shape[1:]
    me = lax.axis_index("head")

    @pl.when(pl.program_id(0) == 0)
    def _():
        copies = []
        for shift in range(count):
            owner = lax.rem(me + count - shift, count)
            if shift:
                source = pieces_ref.at[shift - 1]
            else:
                source = w_hbm.at[pl.ds(pl.multiple_of(me * depth, depth), depth)]
            columns = pl.ds(pl.multiple_of(owner * width, width), width)
            copies.append(pltpu.make_async_copy(source, weight.at[:, columns], sems.at[shift]))
        for copy in copies:
            copy.start()
        for copy in copies:
            copy.wait()

    out_ref[0] = dot(r_ref[...], weight[...]).astype(out_ref.dtype)


def shards(n_seq, n_head, queries, keys, values, gates, ridge, out_weight):
    tokens, head_width = queries.shape
    heads = head_width // HD
    half = heads // 2
    blocks = tokens // SPAN
    pairs = n_seq // 2
    width = out_weight.shape[1]
    tile = SPAN * HD * HD * 2
    hbm = pl.BlockSpec(memory_space=pl.ANY)
    in_vmem = pl.BlockSpec(memory_space=pltpu.VMEM)

    def square(*lead, dtype=f32):
        return pltpu.VMEM((*lead, HD, HD), dtype)

    every, some = heads * blocks, half * blocks
    readout, pieces = pl.pallas_call(
        functools.partial(solve_kernel, n_seq, n_head),
        in_specs=[hbm, hbm, hbm, in_vmem, pl.BlockSpec(memory_space=pltpu.SMEM), hbm],
        out_specs=[in_vmem, hbm],
        out_shape=[
            jax.ShapeDtypeStruct((tokens, head_width), bf16),
            jax.ShapeDtypeStruct((n_head - 1, pairs, 2, head_width // n_seq, width), bf16),
        ],
        scratch_shapes=[
            *[pltpu.VMEM((tokens, head_width), bf16)] * 3,
            pltpu.VMEM((tokens, heads), f32),
            *[square(every, dtype=bf16)] * 3,
            *[square(every)] * 3,
            *[square(some, dtype=bf16)] * 2,
            *[square(some)] * 5,
            square(2, heads),
            square(2, half), square(2, half), square(2, pairs - 1, half), square(2, half), square(2, 2, half),
            pltpu.SemaphoreType.DMA((3,)),
            pltpu.SemaphoreType.DMA((2, n_head - 1)),
            pltpu.SemaphoreType.DMA((2, pairs - 1)),
            pltpu.SemaphoreType.DMA((2,)),
            pltpu.SemaphoreType.DMA((2, 2)),
            pltpu.SemaphoreType.DMA((2, pairs - 1)),
            pltpu.SemaphoreType.DMA((2, pairs - 1)),
            pltpu.SemaphoreType.DMA((2, 2)),
        ],
        compiler_params=pltpu.CompilerParams(
            vmem_limit_bytes=VMEM_BYTES, collective_id=0, has_side_effects=True
        ),
        cost_estimate=pl.CostEstimate(
            flops=heads * blocks * 58 * tile, bytes_accessed=tokens * head_width * 8, transcendentals=0
        ),
        name="solve",
    )(keys, values, queries, gates.T, ridge, out_weight)
    rows = 2 * SPAN
    return pl.pallas_call(
        project_kernel,
        grid=(tokens // rows,),
        in_specs=[pl.BlockSpec((rows, head_width), lambda i: (i, 0)), hbm, hbm],
        out_specs=pl.BlockSpec((1, rows, width * n_head), lambda i: (0, i, 0)),
        out_shape=jax.ShapeDtypeStruct((1, tokens, width * n_head), bf16),
        scratch_shapes=[
            pltpu.VMEM((head_width, width * n_head), bf16),
            pltpu.SemaphoreType.DMA((n_head,)),
        ],
        compiler_params=pltpu.CompilerParams(vmem_limit_bytes=VMEM_BYTES),
        cost_estimate=pl.CostEstimate(
            flops=2 * tokens * head_width * width * n_head,
            bytes_accessed=tokens * width * n_head * 2,
            transcendentals=0,
        ),
        name="project",
    )(readout, out_weight, pieces.reshape(n_head - 1, head_width, width))


def solution(mesh):
    return jax.shard_map(
        functools.partial(shards, mesh.shape["seq"], mesh.shape["head"]),
        mesh=mesh,
        in_specs=(
            P("seq", "head"),
            P("seq", "head"),
            P("seq", "head"),
            P("seq", "head"),
            P("head"),
            P(None, "head"),
        ),
        out_specs=P("head", "seq", None),
        check_vma=False,
    )
```

```python
import functools

import jax
import jax.numpy as jnp
from jax import lax
from jax.experimental import pallas as pl
from jax.experimental.pallas import tpu as pltpu
from jax.sharding import PartitionSpec as P

HD = 128
SPAN = 128
ITERS = 8
EPS = 1e-06
f32 = jnp.float32
bf16 = jnp.bfloat16
VMEM_BYTES = 56 * 1024 * 1024
MESH = pl.DeviceIdType.MESH


def dot(a, b):
    return jnp.dot(a, b, preferred_element_type=f32)


def two_terms(x):
    high = x.astype(bf16)
    return high, (x - high.astype(f32)).astype(bf16)


def row_sum(x):
    return jnp.sum(x, 1, keepdims=True)


def wide(x):
    return jnp.broadcast_to(x, (SPAN, HD))


def solve_kernel(
    n_seq, n_head,
    k_hbm, v_hbm, q_hbm, g_ref, ridge_ref, w_hbm, out_ref, pieces_ref,
    k_ref, v_ref, q_ref, gate_columns, keys_t, keys_w, values_w, scales, gram_local, moment_local,
    gram_high, gram_low, direct, res, sol, norms, images,
    own, mate, chip_sum, slots, give, prior,
    load_sems, piece_sems, plane_sems, chip_sems, mate_sems, send_sems, recv_sems, back_sems,
):
    tokens, head_width = k_ref.shape
    heads = head_width // HD
    half = heads // 2
    blocks = tokens // SPAN
    pairs = n_seq // 2
    me = lax.axis_index("seq")
    group = lax.axis_index("head")
    side = lax.rem(me, 2)
    pair = me // 2
    mate_at = {"seq": me + 1 - 2 * side}
    mine = side * half
    others = (1 - side) * half
    row = lax.broadcasted_iota(jnp.int32, (HD, HD), 0)
    col = lax.broadcasted_iota(jnp.int32, (HD, HD), 1)
    causal = (col <= row).astype(f32).astype(bf16)
    GRAM, MOMENT = 0, 1

    loads = [
        pltpu.make_async_copy(src, dst, load_sems.at[i])
        for i, (src, dst) in enumerate(((k_hbm, k_ref), (v_hbm, v_ref), (q_hbm, q_ref)))
    ]
    for load in loads:
        load.start()

    barrier = pltpu.get_barrier_semaphore()
    pl.semaphore_signal(barrier, inc=1, device_id=mate_at, device_id_type=MESH)
    for off in range(1, pairs):
        target = {"seq": lax.rem(pair + off, pairs) * 2 + side}
        pl.semaphore_signal(barrier, inc=1, device_id=target, device_id_type=MESH)
    for shift in range(1, n_head):
        target = {"head": lax.rem(group + shift, n_head)}
        pl.semaphore_signal(barrier, inc=1, device_id=target, device_id_type=MESH)

    for c in range(blocks):
        rows = pl.ds(c * SPAN, SPAN)
        gate_columns[rows, :] = g_ref[:, rows].T

    def columns_of(h):
        return pl.ds(pl.multiple_of(h * HD, HD), HD)

    def sum_grams(first):
        def one(j, carry):
            h = first + j
            total = jnp.zeros((HD, HD), f32)
            for c in range(blocks):
                n = h * blocks + c
                rows = pl.ds(c * SPAN, SPAN)
                keys = k_ref[rows, columns_of(h)]
                keys_f = keys.astype(f32)
                s = lax.rsqrt(row_sum(keys_f * keys_f) + EPS)
                gates = gate_columns[rows, :]
                gate = row_sum(jnp.where(lax.broadcasted_iota(jnp.int32, gates.shape, 1) == h, gates, 0.0))
                w_value = gate * s
                high, low = two_terms(keys_f * (w_value * s))
                turned = keys.T
                keys_t[n] = turned
                keys_w[n] = high
                scales[n] = wide(w_value)
                gram_local[n] = total
                total += dot(jnp.concatenate([turned, turned], 1), jnp.concatenate([high, low], 0))
            own[GRAM, h] = total
            return carry

        lax.fori_loop(0, half, one, 0)

    def sum_moments(first):
        def one(j, carry):
            h = first + j
            total = jnp.zeros((HD, HD), f32)
            for c in range(blocks):
                n = h * blocks + c
                values = v_ref[pl.ds(c * SPAN, SPAN), columns_of(h)].astype(f32)
                high, low = two_terms(values * scales[n])
                values_w[n] = high
                moment_local[n] = total
                turned = keys_t[n]
                total += dot(jnp.concatenate([turned, turned], 1), jnp.concatenate([high, low], 0))
            own[MOMENT, h] = total
            return carry

        lax.fori_loop(0, half, one, 0)

    def to_mate(kind):
        return pltpu.make_async_remote_copy(
            src_ref=own.at[kind, pl.ds(others, half)], dst_ref=mate.at[kind],
            send_sem=mate_sems.at[kind, 0], recv_sem=mate_sems.at[kind, 1],
            device_id=mate_at, device_id_type=MESH,
        )

    def to_later(kind, off):
        target = {"seq": lax.rem(pair + off, pairs) * 2 + side}
        return pltpu.make_async_remote_copy(
            src_ref=chip_sum.at[kind], dst_ref=slots.at[kind, off - 1],
            send_sem=send_sems.at[kind, off - 1], recv_sem=recv_sems.at[kind, off - 1],
            device_id=target, device_id_type=MESH,
        )

    def to_back(kind):
        return pltpu.make_async_remote_copy(
            src_ref=give.at[kind], dst_ref=prior.at[kind, 1],
            send_sem=back_sems.at[kind, 0], recv_sem=back_sems.at[kind, 1],
            device_id=mate_at, device_id_type=MESH,
        )

    part = pieces_ref.shape[3]
    across = (pair + 1 - 2 * lax.rem(pair, 2), pair + 2 - 4 * lax.rem(pair // 2, 2))
    quarter = 2 * lax.rem(pair + pair // 2, 2)

    def to_head(shift):
        target = lax.rem(group + shift, n_head)
        start = pl.multiple_of(target * head_width + (side * 4 + quarter) * part, part)
        return pltpu.make_async_remote_copy(
            src_ref=w_hbm.at[pl.ds(start, 2 * part)].reshape(2, part, w_hbm.shape[1]),
            dst_ref=pieces_ref.at[shift - 1, side, pl.ds(quarter, 2)],
            send_sem=piece_sems.at[0, shift - 1], recv_sem=piece_sems.at[1, shift - 1],
            device_id={"head": target}, device_id_type=MESH,
        )

    def to_plane(i):
        shared = pieces_ref.at[:, side, quarter + i]
        return pltpu.make_async_remote_copy(
            src_ref=shared, dst_ref=shared,
            send_sem=plane_sems.at[0, i], recv_sem=plane_sems.at[1, i],
            device_id={"seq": across[i] * 2 + side}, device_id_type=MESH,
        )

    def to_chip(i):
        shared = pieces_ref.at[:, side, pl.ds(quarter + i * (2 - 2 * quarter), 2)]
        return pltpu.make_async_remote_copy(
            src_ref=shared, dst_ref=shared,
            send_sem=chip_sems.at[0, i], recv_sem=chip_sems.at[1, i],
            device_id=mate_at, device_id_type=MESH,
        )

    def pass_on(kind):
        to_mate(kind).wait_recv()
        chip_sum[kind] = own[kind, pl.ds(mine, half)] + mate[kind]
        for off in range(1, pairs):
            @pl.when(pair + off < pairs)
            def _():
                to_later(kind, off).start()

    def collect(kind):
        total = jnp.zeros((half, HD, HD), f32)
        give[kind] = total
        for off in range(1, pairs):
            @pl.when(pair >= off)
            def _():
                to_later(kind, off).wait_recv()
                give[kind] = give[kind] + slots[kind, off - 1]
        prior[kind, 0] = give[kind] + side.astype(f32) * mate[kind]
        give[kind] = give[kind] + (1 - side).astype(f32) * own[kind, pl.ds(mine, half)]
        to_back(kind).start()

    loads[0].wait()
    sum_grams(others)
    pl.semaphore_wait(barrier, pairs + n_head - 1)
    to_mate(GRAM).start()
    for shift in range(1, n_head):
        to_head(shift).start()
    sum_grams(mine)
    pass_on(GRAM)
    loads[1].wait()
    sum_moments(others)
    to_mate(MOMENT).start()
    sum_moments(mine)
    pass_on(MOMENT)
    loads[2].wait()
    collect(GRAM)

    def apply(n, at, d, high_ref, low_ref, right_ref, fine=True):
        half_right = jnp.concatenate([high_ref[n], keys_t[at]], 1)
        if fine:
            high, low = two_terms(d)
            first = dot(jnp.concatenate([high, low], 1), jnp.concatenate([half_right, half_right], 0))
        else:
            high = d.astype(bf16)
            first = dot(high, half_right)
        corr = first[:, HD:].astype(bf16) * causal
        if fine:
            left = jnp.concatenate([corr, high], 1)
            right = jnp.concatenate([right_ref[at], low_ref[n]], 0)
        else:
            left, right = corr, right_ref[at]
        second = dot(left, jnp.concatenate([right, right], 1))
        return first[:, :HD] + second[:, :HD]

    units = half * blocks
    behind = units // 2

    def run(p, carry):
        first = mine + p * (others - mine)

        @pl.when(p == 1)
        def _():
            to_back(GRAM).wait_recv()

        def split(kind, j, c, local, low_too=None):
            total = local[(first + j) * blocks + c] + prior[kind, p, j]
            if kind == GRAM:
                total += jnp.where(row == col, ridge_ref[first + j], 0.0)
            gram_high[j * blocks + c], gram_low[j * blocks + c] = two_terms(total)

        def prepare(j, carry):
            for c in range(blocks):
                n = j * blocks + c
                split(GRAM, j, c, gram_local)
                queries = q_ref[pl.ds(c * SPAN, SPAN), columns_of(first + j)].astype(f32)
                square = row_sum(queries * queries)
                scale = lax.rsqrt(square + EPS)
                queries = queries * scale
                res[n] = queries
                direct[n] = queries
                sol[n] = jnp.zeros((SPAN, HD), f32)
                norms[n] = wide(square * scale * scale)
            return carry

        lax.fori_loop(0, half, prepare, 0)

        def multiply(n, fine=True):
            images[n] = apply(n, first * blocks + n, direct[n], gram_high, gram_low, keys_w, fine)

        def update(n, last=False):
            d = direct[n]
            image = images[n]
            now = norms[n]
            step = now / (row_sum(d * image) + EPS)
            sol[n] = sol[n] + step * d
            if last:
                return
            r = res[n] - step * image
            res[n] = r
            following = wide(row_sum(r * r))
            norms[n] = following
            direct[n] = r + following / (now + EPS) * d

        def iteration(last=False, before_last=False):
            for n in range(behind):
                multiply(n, not last)
                update(behind + n, last)
            for n in range(behind):
                update(n, last)
                if not last:
                    multiply(behind + n, not before_last)

        for n in range(behind):
            multiply(behind + n)

        def sweep(i, carry):
            iteration()
            iteration()

            @pl.when((p == 0) & (i == 1))
            def _():
                for shift in range(1, n_head):
                    to_head(shift).wait_recv()
                for which in range(2):
                    to_plane(which).start()
                to_chip(0).start()

            @pl.when((p == 1) & (i == 0))
            def _():
                for which in range(2):
                    to_plane(which).wait_recv()
                to_chip(1).start()

            return carry

        lax.fori_loop(0, (ITERS - 2) // 2, sweep, 0)
        iteration(before_last=True)
        iteration(last=True)

        @pl.when(p == 0)
        def _():
            collect(MOMENT)

        @pl.when(p == 1)
        def _():
            to_back(MOMENT).wait_recv()

        def finish(j, carry):
            for c in range(blocks):
                split(MOMENT, j, c, moment_local)
            for c in range(blocks):
                n = j * blocks + c
                out_ref[pl.ds(c * SPAN, SPAN), columns_of(first + j)] = apply(
                    n, first * blocks + n, sol[n], gram_high, gram_low, values_w
                ).astype(out_ref.dtype)
            return carry

        lax.fori_loop(0, half, finish, 0)
        return carry

    lax.fori_loop(0, 2, run, 0)
    for kind in (GRAM, MOMENT):
        to_mate(kind).wait_send()
        to_back(kind).wait_send()
        for off in range(1, pairs):
            @pl.when(pair + off < pairs)
            def _():
                to_later(kind, off).wait_send()
    for shift in range(1, n_head):
        to_head(shift).wait_send()
    for i in range(2):
        to_plane(i).wait_send()
        to_chip(i).wait()


def project_kernel(r_ref, w_hbm, pieces_ref, out_ref, weight, sems):
    count = pieces_ref.shape[0] + 1
    depth, width = pieces_ref.shape[1:]
    me = lax.axis_index("head")

    @pl.when(pl.program_id(0) == 0)
    def _():
        copies = []
        for shift in range(count):
            owner = lax.rem(me + count - shift, count)
            if shift:
                source = pieces_ref.at[shift - 1]
            else:
                source = w_hbm.at[pl.ds(pl.multiple_of(me * depth, depth), depth)]
            columns = pl.ds(pl.multiple_of(owner * width, width), width)
            copies.append(pltpu.make_async_copy(source, weight.at[:, columns], sems.at[shift]))
        for copy in copies:
            copy.start()
        for copy in copies:
            copy.wait()

    out_ref[0] = dot(r_ref[...], weight[...]).astype(out_ref.dtype)


def shards(n_seq, n_head, queries, keys, values, gates, ridge, out_weight):
    tokens, head_width = queries.shape
    heads = head_width // HD
    half = heads // 2
    blocks = tokens // SPAN
    pairs = n_seq // 2
    width = out_weight.shape[1]
    tile = SPAN * HD * HD * 2
    hbm = pl.BlockSpec(memory_space=pl.ANY)
    in_vmem = pl.BlockSpec(memory_space=pltpu.VMEM)

    def square(*lead, dtype=f32):
        return pltpu.VMEM((*lead, HD, HD), dtype)

    every, some = heads * blocks, half * blocks
    readout, pieces = pl.pallas_call(
        functools.partial(solve_kernel, n_seq, n_head),
        in_specs=[hbm, hbm, hbm, in_vmem, pl.BlockSpec(memory_space=pltpu.SMEM), hbm],
        out_specs=[in_vmem, hbm],
        out_shape=[
            jax.ShapeDtypeStruct((tokens, head_width), bf16),
            jax.ShapeDtypeStruct((n_head - 1, 2, 4, head_width // 8, width), bf16),
        ],
        scratch_shapes=[
            *[pltpu.VMEM((tokens, head_width), bf16)] * 3,
            pltpu.VMEM((tokens, heads), f32),
            *[square(every, dtype=bf16)] * 3,
            *[square(every)] * 3,
            *[square(some, dtype=bf16)] * 2,
            *[square(some)] * 5,
            square(2, heads),
            square(2, half), square(2, half), square(2, pairs - 1, half), square(2, half), square(2, 2, half),
            pltpu.SemaphoreType.DMA((3,)),
            pltpu.SemaphoreType.DMA((2, n_head - 1)),
            pltpu.SemaphoreType.DMA((2, 2)),
            pltpu.SemaphoreType.DMA((2, 2)),
            pltpu.SemaphoreType.DMA((2, 2)),
            pltpu.SemaphoreType.DMA((2, pairs - 1)),
            pltpu.SemaphoreType.DMA((2, pairs - 1)),
            pltpu.SemaphoreType.DMA((2, 2)),
        ],
        compiler_params=pltpu.CompilerParams(
            vmem_limit_bytes=VMEM_BYTES, collective_id=0, has_side_effects=True
        ),
        cost_estimate=pl.CostEstimate(
            flops=heads * blocks * 58 * tile, bytes_accessed=tokens * head_width * 8, transcendentals=0
        ),
        name="solve",
    )(keys, values, queries, gates.T, ridge, out_weight)
    rows = 2 * SPAN
    return pl.pallas_call(
        project_kernel,
        grid=(tokens // rows,),
        in_specs=[pl.BlockSpec((rows, head_width), lambda i: (i, 0)), hbm, hbm],
        out_specs=pl.BlockSpec((1, rows, width * n_head), lambda i: (0, i, 0)),
        out_shape=jax.ShapeDtypeStruct((1, tokens, width * n_head), bf16),
        scratch_shapes=[
            pltpu.VMEM((head_width, width * n_head), bf16),
            pltpu.SemaphoreType.DMA((n_head,)),
        ],
        compiler_params=pltpu.CompilerParams(vmem_limit_bytes=VMEM_BYTES),
        cost_estimate=pl.CostEstimate(
            flops=2 * tokens * head_width * width * n_head,
            bytes_accessed=tokens * width * n_head * 2,
            transcendentals=0,
        ),
        name="project",
    )(readout, out_weight, pieces.reshape(n_head - 1, head_width, width))


def solution(mesh):
    return jax.shard_map(
        functools.partial(shards, mesh.shape["seq"], mesh.shape["head"]),
        mesh=mesh,
        in_specs=(
            P("seq", "head"),
            P("seq", "head"),
            P("seq", "head"),
            P("seq", "head"),
            P("head"),
            P(None, "head"),
        ),
        out_specs=P("head", "seq", None),
        check_vma=False,
    )
```

```python
import functools

import jax
import jax.numpy as jnp
from jax import lax
from jax.experimental import pallas as pl
from jax.experimental.pallas import tpu as pltpu
from jax.sharding import PartitionSpec as P

HD = 128
SPAN = 128
ITERS = 8
EPS = 1e-06
f32 = jnp.float32
bf16 = jnp.bfloat16
VMEM_BYTES = 56 * 1024 * 1024
MESH = pl.DeviceIdType.MESH


def dot(a, b):
    return jnp.dot(a, b, preferred_element_type=f32)


def two_terms(x):
    high = x.astype(bf16)
    return high, (x - high.astype(f32)).astype(bf16)


def row_sum(x):
    return jnp.sum(x, 1, keepdims=True)


def wide(x):
    return jnp.broadcast_to(x, (SPAN, HD))


def solve_kernel(
    n_seq, n_head,
    k_hbm, v_hbm, q_hbm, g_ref, ridge_ref, w_hbm, out_ref, pieces_ref,
    k_ref, v_ref, q_ref, gate_columns, keys_t, keys_w, values_w, scales, gram_local, moment_local,
    gram_high, gram_low, direct, res, sol, norms, images,
    own, mate, chip_gram, chip_moment, gram_slots, moment_slots, give, prior,
    load_sems, piece_sems, plane_sems, chip_sems, mate_sems, send_sems, recv_sems, back_sems,
):
    tokens, head_width = k_ref.shape
    heads = head_width // HD
    half = heads // 2
    blocks = tokens // SPAN
    pairs = n_seq // 2
    me = lax.axis_index("seq")
    group = lax.axis_index("head")
    side = lax.rem(me, 2)
    pair = me // 2
    mate_at = {"seq": me + 1 - 2 * side}
    mine = side * half
    others = (1 - side) * half
    row = lax.broadcasted_iota(jnp.int32, (HD, HD), 0)
    col = lax.broadcasted_iota(jnp.int32, (HD, HD), 1)
    causal = (col <= row).astype(f32).astype(bf16)
    GRAM, MOMENT = 0, 1
    chip_sums, slots = (chip_gram, chip_moment), (gram_slots, moment_slots)

    loads = [
        pltpu.make_async_copy(src, dst, load_sems.at[i])
        for i, (src, dst) in enumerate(((k_hbm, k_ref), (v_hbm, v_ref), (q_hbm, q_ref)))
    ]
    for load in loads:
        load.start()

    barrier = pltpu.get_barrier_semaphore()
    pl.semaphore_signal(barrier, inc=1, device_id=mate_at, device_id_type=MESH)
    for off in range(1, pairs):
        target = {"seq": lax.rem(pair + off, pairs) * 2 + side}
        pl.semaphore_signal(barrier, inc=1, device_id=target, device_id_type=MESH)
    for shift in range(1, n_head):
        target = {"head": lax.rem(group + shift, n_head)}
        pl.semaphore_signal(barrier, inc=1, device_id=target, device_id_type=MESH)

    for c in range(blocks):
        rows = pl.ds(c * SPAN, SPAN)
        gate_columns[rows, :] = g_ref[:, rows].T

    def columns_of(h):
        return pl.ds(pl.multiple_of(h * HD, HD), HD)

    def sum_grams(first):
        def one(j, carry):
            h = first + j
            total = jnp.zeros((HD, HD), f32)
            for c in range(blocks):
                n = h * blocks + c
                rows = pl.ds(c * SPAN, SPAN)
                keys = k_ref[rows, columns_of(h)]
                keys_f = keys.astype(f32)
                s = lax.rsqrt(row_sum(keys_f * keys_f) + EPS)
                gates = gate_columns[rows, :]
                gate = row_sum(jnp.where(lax.broadcasted_iota(jnp.int32, gates.shape, 1) == h, gates, 0.0))
                w_value = gate * s
                high, low = two_terms(keys_f * (w_value * s))
                turned = keys.T
                keys_t[n] = turned
                keys_w[n] = high
                scales[n] = wide(w_value)
                gram_local[n] = total
                total += dot(jnp.concatenate([turned, turned], 1), jnp.concatenate([high, low], 0))
            own[GRAM, h] = total
            return carry

        lax.fori_loop(0, half, one, 0)

    def sum_moments(first):
        def one(j, carry):
            h = first + j
            total = jnp.zeros((HD, HD), f32)
            for c in range(blocks):
                n = h * blocks + c
                values = v_ref[pl.ds(c * SPAN, SPAN), columns_of(h)].astype(f32)
                high, low = two_terms(values * scales[n])
                values_w[n] = high
                moment_local[n] = total
                turned = keys_t[n]
                total += dot(jnp.concatenate([turned, turned], 1), jnp.concatenate([high, low], 0))
            own[MOMENT, h] = total
            return carry

        lax.fori_loop(0, half, one, 0)

    def to_mate(kind):
        return pltpu.make_async_remote_copy(
            src_ref=own.at[kind, pl.ds(others, half)], dst_ref=mate.at[kind],
            send_sem=mate_sems.at[kind, 0], recv_sem=mate_sems.at[kind, 1],
            device_id=mate_at, device_id_type=MESH,
        )

    def to_later(kind, off):
        target = {"seq": lax.rem(pair + off, pairs) * 2 + side}
        return pltpu.make_async_remote_copy(
            src_ref=chip_sums[kind], dst_ref=slots[kind].at[off - 1],
            send_sem=send_sems.at[kind, off - 1], recv_sem=recv_sems.at[kind, off - 1],
            device_id=target, device_id_type=MESH,
        )

    def to_back(kind):
        return pltpu.make_async_remote_copy(
            src_ref=give.at[kind], dst_ref=prior.at[kind, 1],
            send_sem=back_sems.at[kind, 0], recv_sem=back_sems.at[kind, 1],
            device_id=mate_at, device_id_type=MESH,
        )

    part = pieces_ref.shape[3]
    across = (pair + 1 - 2 * lax.rem(pair, 2), pair + 2 - 4 * lax.rem(pair // 2, 2))
    quarter = 2 * lax.rem(pair + pair // 2, 2)

    def to_head(shift):
        target = lax.rem(group + shift, n_head)
        start = pl.multiple_of(target * head_width + (side * 4 + quarter) * part, part)
        return pltpu.make_async_remote_copy(
            src_ref=w_hbm.at[pl.ds(start, 2 * part)].reshape(2, part, w_hbm.shape[1]),
            dst_ref=pieces_ref.at[shift - 1, side, pl.ds(quarter, 2)],
            send_sem=piece_sems.at[0, shift - 1], recv_sem=piece_sems.at[1, shift - 1],
            device_id={"head": target}, device_id_type=MESH,
        )

    def to_plane(i):
        shared = pieces_ref.at[:, side, quarter + i]
        return pltpu.make_async_remote_copy(
            src_ref=shared, dst_ref=shared,
            send_sem=plane_sems.at[0, i], recv_sem=plane_sems.at[1, i],
            device_id={"seq": across[i] * 2 + side}, device_id_type=MESH,
        )

    def to_chip(i):
        shared = pieces_ref.at[:, side, pl.ds(quarter + i * (2 - 2 * quarter), 2)]
        return pltpu.make_async_remote_copy(
            src_ref=shared, dst_ref=shared,
            send_sem=chip_sems.at[0, i], recv_sem=chip_sems.at[1, i],
            device_id=mate_at, device_id_type=MESH,
        )

    def pass_on(kind):
        to_mate(kind).wait_recv()
        chip = own[kind, pl.ds(mine, half)] + mate[kind]
        chip_sums[kind][...] = chip.astype(chip_sums[kind].dtype)
        for off in range(1, pairs):
            @pl.when(pair + off < pairs)
            def _():
                to_later(kind, off).start()

    def collect(kind):
        total = jnp.zeros((half, HD, HD), f32)
        give[kind] = total
        for off in range(1, pairs):
            @pl.when(pair >= off)
            def _():
                to_later(kind, off).wait_recv()
                give[kind] = give[kind] + slots[kind][off - 1].astype(f32)
        prior[kind, 0] = give[kind] + side.astype(f32) * mate[kind]
        give[kind] = give[kind] + (1 - side).astype(f32) * own[kind, pl.ds(mine, half)]
        to_back(kind).start()

    loads[0].wait()
    sum_grams(others)
    pl.semaphore_wait(barrier, pairs + n_head - 1)
    to_mate(GRAM).start()
    sum_grams(mine)
    pass_on(GRAM)
    for shift in range(1, n_head):
        to_head(shift).start()
    loads[1].wait()
    sum_moments(others)
    to_mate(MOMENT).start()
    sum_moments(mine)
    loads[2].wait()
    collect(GRAM)

    def apply(n, at, d, high_ref, low_ref, right_ref, fine=True):
        half_right = jnp.concatenate([high_ref[n], keys_t[at]], 1)
        if fine:
            high, low = two_terms(d)
            first = dot(jnp.concatenate([high, low], 1), jnp.concatenate([half_right, half_right], 0))
        else:
            high = d.astype(bf16)
            first = dot(high, half_right)
        corr = first[:, HD:].astype(bf16) * causal
        if fine:
            left = jnp.concatenate([corr, high], 1)
            right = jnp.concatenate([right_ref[at], low_ref[n]], 0)
        else:
            left, right = corr, right_ref[at]
        second = dot(left, jnp.concatenate([right, right], 1))
        return first[:, :HD] + second[:, :HD]

    units = half * blocks
    behind = units // 2

    def run(p, carry):
        first = mine + p * (others - mine)

        @pl.when(p == 1)
        def _():
            to_back(GRAM).wait_recv()

        def split(kind, j, c, local, low_too=None):
            total = local[(first + j) * blocks + c] + prior[kind, p, j]
            if kind == GRAM:
                total += jnp.where(row == col, ridge_ref[first + j], 0.0)
            gram_high[j * blocks + c], gram_low[j * blocks + c] = two_terms(total)

        def prepare(j, carry):
            for c in range(blocks):
                n = j * blocks + c
                split(GRAM, j, c, gram_local)
                queries = q_ref[pl.ds(c * SPAN, SPAN), columns_of(first + j)].astype(f32)
                square = row_sum(queries * queries)
                scale = lax.rsqrt(square + EPS)
                queries = queries * scale
                res[n] = queries
                direct[n] = queries
                sol[n] = jnp.zeros((SPAN, HD), f32)
                norms[n] = wide(square * scale * scale)
            return carry

        lax.fori_loop(0, half, prepare, 0)

        def multiply(n, fine=True):
            images[n] = apply(n, first * blocks + n, direct[n], gram_high, gram_low, keys_w, fine)

        def update(n, last=False):
            d = direct[n]
            image = images[n]
            now = norms[n]
            step = now / (row_sum(d * image) + EPS)
            sol[n] = sol[n] + step * d
            if last:
                return
            r = res[n] - step * image
            res[n] = r
            following = wide(row_sum(r * r))
            norms[n] = following
            direct[n] = r + following / (now + EPS) * d

        def iteration(last=False, before_last=False):
            for n in range(behind):
                multiply(n, not last)
                update(behind + n, last)
            for n in range(behind):
                update(n, last)
                if not last:
                    multiply(behind + n, not before_last)

        for n in range(behind):
            multiply(behind + n)

        def sweep(i, carry):
            iteration()
            iteration()

            @pl.when((p == 0) & (i == 0))
            def _():
                pass_on(MOMENT)

            @pl.when((p == 1) & (i == 2))
            def _():
                for which in range(2):
                    to_plane(which).wait_recv()
                to_chip(1).start()

            return carry

        lax.fori_loop(0, (ITERS - 2) // 2, sweep, 0)
        iteration(before_last=True)
        iteration(last=True)

        @pl.when(p == 0)
        def _():
            collect(MOMENT)
            for shift in range(1, n_head):
                to_head(shift).wait_recv()
            for which in range(2):
                to_plane(which).start()
            to_chip(0).start()

        @pl.when(p == 1)
        def _():
            to_back(MOMENT).wait_recv()

        def finish(j, carry):
            for c in range(blocks):
                split(MOMENT, j, c, moment_local)
            for c in range(blocks):
                n = j * blocks + c
                out_ref[pl.ds(c * SPAN, SPAN), columns_of(first + j)] = apply(
                    n, first * blocks + n, sol[n], gram_high, gram_low, values_w
                ).astype(out_ref.dtype)
            return carry

        lax.fori_loop(0, half, finish, 0)
        return carry

    lax.fori_loop(0, 2, run, 0)
    for kind in (GRAM, MOMENT):
        to_mate(kind).wait_send()
        to_back(kind).wait_send()
        for off in range(1, pairs):
            @pl.when(pair + off < pairs)
            def _():
                to_later(kind, off).wait_send()
    for shift in range(1, n_head):
        to_head(shift).wait_send()
    for i in range(2):
        to_plane(i).wait_send()
        to_chip(i).wait()


def project_kernel(r_ref, w_hbm, pieces_ref, out_ref, weight, sems):
    count = pieces_ref.shape[0] + 1
    depth, width = pieces_ref.shape[1:]
    me = lax.axis_index("head")

    @pl.when(pl.program_id(0) == 0)
    def _():
        copies = []
        for shift in range(count):
            owner = lax.rem(me + count - shift, count)
            if shift:
                source = pieces_ref.at[shift - 1]
            else:
                source = w_hbm.at[pl.ds(pl.multiple_of(me * depth, depth), depth)]
            columns = pl.ds(pl.multiple_of(owner * width, width), width)
            copies.append(pltpu.make_async_copy(source, weight.at[:, columns], sems.at[shift]))
        for copy in copies:
            copy.start()
        for copy in copies:
            copy.wait()

    out_ref[0] = dot(r_ref[...], weight[...]).astype(out_ref.dtype)


def shards(n_seq, n_head, queries, keys, values, gates, ridge, out_weight):
    tokens, head_width = queries.shape
    heads = head_width // HD
    half = heads // 2
    blocks = tokens // SPAN
    pairs = n_seq // 2
    width = out_weight.shape[1]
    tile = SPAN * HD * HD * 2
    hbm = pl.BlockSpec(memory_space=pl.ANY)
    in_vmem = pl.BlockSpec(memory_space=pltpu.VMEM)

    def square(*lead, dtype=f32):
        return pltpu.VMEM((*lead, HD, HD), dtype)

    every, some = heads * blocks, half * blocks
    readout, pieces = pl.pallas_call(
        functools.partial(solve_kernel, n_seq, n_head),
        in_specs=[hbm, hbm, hbm, in_vmem, pl.BlockSpec(memory_space=pltpu.SMEM), hbm],
        out_specs=[in_vmem, hbm],
        out_shape=[
            jax.ShapeDtypeStruct((tokens, head_width), bf16),
            jax.ShapeDtypeStruct((n_head - 1, 2, 4, head_width // 8, width), bf16),
        ],
        scratch_shapes=[
            *[pltpu.VMEM((tokens, head_width), bf16)] * 3,
            pltpu.VMEM((tokens, heads), f32),
            *[square(every, dtype=bf16)] * 3,
            *[square(every)] * 3,
            *[square(some, dtype=bf16)] * 2,
            *[square(some)] * 5,
            square(2, heads),
            square(2, half), square(half), square(half, dtype=bf16),
            square(pairs - 1, half), square(pairs - 1, half, dtype=bf16),
            square(2, half), square(2, 2, half),
            pltpu.SemaphoreType.DMA((3,)),
            pltpu.SemaphoreType.DMA((2, n_head - 1)),
            pltpu.SemaphoreType.DMA((2, 2)),
            pltpu.SemaphoreType.DMA((2, 2)),
            pltpu.SemaphoreType.DMA((2, 2)),
            pltpu.SemaphoreType.DMA((2, pairs - 1)),
            pltpu.SemaphoreType.DMA((2, pairs - 1)),
            pltpu.SemaphoreType.DMA((2, 2)),
        ],
        compiler_params=pltpu.CompilerParams(
            vmem_limit_bytes=VMEM_BYTES, collective_id=0, has_side_effects=True
        ),
        cost_estimate=pl.CostEstimate(
            flops=heads * blocks * 58 * tile, bytes_accessed=tokens * head_width * 8, transcendentals=0
        ),
        name="solve",
    )(keys, values, queries, gates.T, ridge, out_weight)
    rows = 2 * SPAN
    return pl.pallas_call(
        project_kernel,
        grid=(tokens // rows,),
        in_specs=[pl.BlockSpec((rows, head_width), lambda i: (i, 0)), hbm, hbm],
        out_specs=pl.BlockSpec((1, rows, width * n_head), lambda i: (0, i, 0)),
        out_shape=jax.ShapeDtypeStruct((1, tokens, width * n_head), bf16),
        scratch_shapes=[
            pltpu.VMEM((head_width, width * n_head), bf16),
            pltpu.SemaphoreType.DMA((n_head,)),
        ],
        compiler_params=pltpu.CompilerParams(vmem_limit_bytes=VMEM_BYTES),
        cost_estimate=pl.CostEstimate(
            flops=2 * tokens * head_width * width * n_head,
            bytes_accessed=tokens * width * n_head * 2,
            transcendentals=0,
        ),
        name="project",
    )(readout, out_weight, pieces.reshape(n_head - 1, head_width, width))


def solution(mesh):
    return jax.shard_map(
        functools.partial(shards, mesh.shape["seq"], mesh.shape["head"]),
        mesh=mesh,
        in_specs=(
            P("seq", "head"),
            P("seq", "head"),
            P("seq", "head"),
            P("seq", "head"),
            P("head"),
            P(None, "head"),
        ),
        out_specs=P("head", "seq", None),
        check_vma=False,
    )
```

```python
import functools

import jax
import jax.numpy as jnp
from jax import lax
from jax.experimental import pallas as pl
from jax.experimental.pallas import tpu as pltpu
from jax.sharding import PartitionSpec as P

HD = 128
SPAN = 128
ITERS = 8
EPS = 1e-06
f32 = jnp.float32
bf16 = jnp.bfloat16
VMEM_BYTES = 56 * 1024 * 1024
MESH = pl.DeviceIdType.MESH
PROJECT_ROWS = 256


def dot(a, b):
    return jnp.dot(a, b, preferred_element_type=f32)


def two_terms(x):
    high = x.astype(bf16)
    return high, (x - high.astype(f32)).astype(bf16)


def row_sum(x):
    return jnp.sum(x, 1, keepdims=True)


def wide(x):
    return jnp.broadcast_to(x, (SPAN, HD))


def solve_kernel(
    n_seq, n_head,
    k_hbm, v_hbm, q_hbm, g_ref, ridge_ref, w_hbm, out_ref, pieces_ref,
    k_ref, v_ref, q_ref, gate_columns, keys_t, keys_w, values_w, scales, gram_local, moment_local,
    gram_high, gram_low, direct, res, sol, norms, images,
    own, mate, chip_gram, chip_moment, gram_slots, moment_slots, give, prior,
    load_sems, piece_sems, plane_sems, chip_sems, mate_sems, send_sems, recv_sems, back_sems,
):
    tokens, head_width = k_ref.shape
    heads = head_width // HD
    half = heads // 2
    blocks = tokens // SPAN
    pairs = n_seq // 2
    me = lax.axis_index("seq")
    group = lax.axis_index("head")
    side = lax.rem(me, 2)
    pair = me // 2
    mate_at = {"seq": me + 1 - 2 * side}
    mine = side * half
    others = (1 - side) * half
    row = lax.broadcasted_iota(jnp.int32, (HD, HD), 0)
    col = lax.broadcasted_iota(jnp.int32, (HD, HD), 1)
    causal = (col <= row).astype(f32).astype(bf16)
    GRAM, MOMENT = 0, 1
    chip_sums, slots = (chip_gram, chip_moment), (gram_slots, moment_slots)

    loads = [
        pltpu.make_async_copy(src, dst, load_sems.at[i])
        for i, (src, dst) in enumerate(((k_hbm, k_ref), (v_hbm, v_ref), (q_hbm, q_ref)))
    ]
    for load in loads:
        load.start()

    barrier = pltpu.get_barrier_semaphore()
    pl.semaphore_signal(barrier, inc=1, device_id=mate_at, device_id_type=MESH)
    for off in range(1, pairs):
        target = {"seq": lax.rem(pair + off, pairs) * 2 + side}
        pl.semaphore_signal(barrier, inc=1, device_id=target, device_id_type=MESH)
    for shift in range(1, n_head):
        target = {"head": lax.rem(group + shift, n_head)}
        pl.semaphore_signal(barrier, inc=1, device_id=target, device_id_type=MESH)

    for c in range(blocks):
        rows = pl.ds(c * SPAN, SPAN)
        gate_columns[rows, :] = g_ref[:, rows].T

    def columns_of(h):
        return pl.ds(pl.multiple_of(h * HD, HD), HD)

    def sum_grams(first):
        def one(j, carry):
            h = first + j
            total = jnp.zeros((HD, HD), f32)
            for c in range(blocks):
                n = h * blocks + c
                rows = pl.ds(c * SPAN, SPAN)
                keys = k_ref[rows, columns_of(h)]
                keys_f = keys.astype(f32)
                s = lax.rsqrt(row_sum(keys_f * keys_f) + EPS)
                gates = gate_columns[rows, :]
                gate = row_sum(jnp.where(lax.broadcasted_iota(jnp.int32, gates.shape, 1) == h, gates, 0.0))
                w_value = gate * s
                high, low = two_terms(keys_f * (w_value * s))
                turned = keys.T
                keys_t[n] = turned
                keys_w[n] = high
                scales[n] = wide(w_value)
                gram_local[n] = total
                total += dot(jnp.concatenate([turned, turned], 1), jnp.concatenate([high, low], 0))
            own[GRAM, h] = total
            return carry

        lax.fori_loop(0, half, one, 0)

    def sum_moments(first):
        def one(j, carry):
            h = first + j
            total = jnp.zeros((HD, HD), f32)
            for c in range(blocks):
                n = h * blocks + c
                values = v_ref[pl.ds(c * SPAN, SPAN), columns_of(h)].astype(f32)
                high, low = two_terms(values * scales[n])
                values_w[n] = high
                moment_local[n] = total
                turned = keys_t[n]
                total += dot(jnp.concatenate([turned, turned], 1), jnp.concatenate([high, low], 0))
            own[MOMENT, h] = total
            return carry

        lax.fori_loop(0, half, one, 0)

    def to_mate(kind):
        return pltpu.make_async_remote_copy(
            src_ref=own.at[kind, pl.ds(others, half)], dst_ref=mate.at[kind],
            send_sem=mate_sems.at[kind, 0], recv_sem=mate_sems.at[kind, 1],
            device_id=mate_at, device_id_type=MESH,
        )

    def to_later(kind, off):
        target = {"seq": lax.rem(pair + off, pairs) * 2 + side}
        return pltpu.make_async_remote_copy(
            src_ref=chip_sums[kind], dst_ref=slots[kind].at[off - 1],
            send_sem=send_sems.at[kind, off - 1], recv_sem=recv_sems.at[kind, off - 1],
            device_id=target, device_id_type=MESH,
        )

    def to_back(kind):
        return pltpu.make_async_remote_copy(
            src_ref=give.at[kind], dst_ref=prior.at[kind, 1],
            send_sem=back_sems.at[kind, 0], recv_sem=back_sems.at[kind, 1],
            device_id=mate_at, device_id_type=MESH,
        )

    part = pieces_ref.shape[3]
    across = (pair + 1 - 2 * lax.rem(pair, 2), pair + 2 - 4 * lax.rem(pair // 2, 2))
    quarter = 2 * lax.rem(pair + pair // 2, 2)

    def to_head(shift):
        target = lax.rem(group + shift, n_head)
        start = pl.multiple_of(target * head_width + (side * 4 + quarter) * part, part)
        return pltpu.make_async_remote_copy(
            src_ref=w_hbm.at[pl.ds(start, 2 * part)].reshape(2, part, w_hbm.shape[1]),
            dst_ref=pieces_ref.at[shift - 1, side, pl.ds(quarter, 2)],
            send_sem=piece_sems.at[0, shift - 1], recv_sem=piece_sems.at[1, shift - 1],
            device_id={"head": target}, device_id_type=MESH,
        )

    def to_plane(i):
        shared = pieces_ref.at[:, side, quarter + i]
        return pltpu.make_async_remote_copy(
            src_ref=shared, dst_ref=shared,
            send_sem=plane_sems.at[0, i], recv_sem=plane_sems.at[1, i],
            device_id={"seq": across[i] * 2 + side}, device_id_type=MESH,
        )

    def to_chip(i):
        shared = pieces_ref.at[:, side, pl.ds(quarter + i * (2 - 2 * quarter), 2)]
        return pltpu.make_async_remote_copy(
            src_ref=shared, dst_ref=shared,
            send_sem=chip_sems.at[0, i], recv_sem=chip_sems.at[1, i],
            device_id=mate_at, device_id_type=MESH,
        )

    def pass_on(kind):
        to_mate(kind).wait_recv()
        chip = own[kind, pl.ds(mine, half)] + mate[kind]
        chip_sums[kind][...] = chip.astype(chip_sums[kind].dtype)
        for off in range(1, pairs):
            @pl.when(pair + off < pairs)
            def _():
                to_later(kind, off).start()

    def collect(kind):
        total = jnp.zeros((half, HD, HD), f32)
        give[kind] = total
        for off in range(1, pairs):
            @pl.when(pair >= off)
            def _():
                to_later(kind, off).wait_recv()
                give[kind] = give[kind] + slots[kind][off - 1].astype(f32)
        prior[kind, 0] = give[kind] + side.astype(f32) * mate[kind]
        give[kind] = give[kind] + (1 - side).astype(f32) * own[kind, pl.ds(mine, half)]
        to_back(kind).start()

    loads[0].wait()
    sum_grams(others)
    pl.semaphore_wait(barrier, pairs + n_head - 1)
    to_mate(GRAM).start()
    sum_grams(mine)
    pass_on(GRAM)
    for shift in range(1, n_head):
        to_head(shift).start()
    loads[1].wait()
    sum_moments(others)
    to_mate(MOMENT).start()
    sum_moments(mine)
    loads[2].wait()
    collect(GRAM)

    def apply(n, at, d, high_ref, low_ref, right_ref, fine=True):
        half_right = jnp.concatenate([high_ref[n], keys_t[at]], 1)
        if fine:
            high, low = two_terms(d)
            first = dot(jnp.concatenate([high, low], 1), jnp.concatenate([half_right, half_right], 0))
        else:
            high = d.astype(bf16)
            first = dot(high, half_right)
        corr = first[:, HD:].astype(bf16) * causal
        if fine:
            left = jnp.concatenate([corr, high], 1)
            right = jnp.concatenate([right_ref[at], low_ref[n]], 0)
        else:
            left, right = corr, right_ref[at]
        second = dot(left, jnp.concatenate([right, right], 1))
        return first[:, :HD] + second[:, :HD]

    units = half * blocks
    behind = units // 2

    def run(p, carry):
        first = mine + p * (others - mine)

        @pl.when(p == 1)
        def _():
            to_back(GRAM).wait_recv()

        def split(kind, j, c, local, low_too=None):
            total = local[(first + j) * blocks + c] + prior[kind, p, j]
            if kind == GRAM:
                total += jnp.where(row == col, ridge_ref[first + j], 0.0)
            gram_high[j * blocks + c], gram_low[j * blocks + c] = two_terms(total)

        def prepare(j, carry):
            for c in range(blocks):
                n = j * blocks + c
                split(GRAM, j, c, gram_local)
                queries = q_ref[pl.ds(c * SPAN, SPAN), columns_of(first + j)].astype(f32)
                square = row_sum(queries * queries)
                scale = lax.rsqrt(square + EPS)
                queries = queries * scale
                res[n] = queries
                direct[n] = queries
                sol[n] = jnp.zeros((SPAN, HD), f32)
                norms[n] = wide(square * scale * scale)
            return carry

        lax.fori_loop(0, half, prepare, 0)

        def multiply(n, fine=True):
            images[n] = apply(n, first * blocks + n, direct[n], gram_high, gram_low, keys_w, fine)

        def update(n, last=False):
            d = direct[n]
            image = images[n]
            now = norms[n]
            step = now / (row_sum(d * image) + EPS)
            sol[n] = sol[n] + step * d
            if last:
                return
            r = res[n] - step * image
            res[n] = r
            following = wide(row_sum(r * r))
            norms[n] = following
            direct[n] = r + following / (now + EPS) * d

        def iteration(last=False, before_last=False):
            for n in range(behind):
                multiply(n, not last)
                update(behind + n, last)
            for n in range(behind):
                update(n, last)
                if not last:
                    multiply(behind + n, not before_last)

        for n in range(behind):
            multiply(behind + n)

        def sweep(i, carry):
            iteration()
            iteration()

            @pl.when((p == 0) & (i == 0))
            def _():
                pass_on(MOMENT)

            @pl.when((p == 1) & (i == 2))
            def _():
                for which in range(2):
                    to_plane(which).wait_recv()
                to_chip(1).start()

            return carry

        lax.fori_loop(0, (ITERS - 2) // 2, sweep, 0)
        iteration(before_last=True)
        iteration(last=True)

        @pl.when(p == 0)
        def _():
            collect(MOMENT)
            for shift in range(1, n_head):
                to_head(shift).wait_recv()
            for which in range(2):
                to_plane(which).start()
            to_chip(0).start()

        @pl.when(p == 1)
        def _():
            to_back(MOMENT).wait_recv()

        def finish(j, carry):
            for c in range(blocks):
                split(MOMENT, j, c, moment_local)
            for c in range(blocks):
                n = j * blocks + c
                out_ref[pl.ds(c * SPAN, SPAN), columns_of(first + j)] = apply(
                    n, first * blocks + n, sol[n], gram_high, gram_low, values_w
                ).astype(out_ref.dtype)
            return carry

        lax.fori_loop(0, half, finish, 0)
        return carry

    lax.fori_loop(0, 2, run, 0)
    for kind in (GRAM, MOMENT):
        to_mate(kind).wait_send()
        to_back(kind).wait_send()
        for off in range(1, pairs):
            @pl.when(pair + off < pairs)
            def _():
                to_later(kind, off).wait_send()
    for shift in range(1, n_head):
        to_head(shift).wait_send()
    for i in range(2):
        to_plane(i).wait_send()
        to_chip(i).wait()


def project_kernel(r_hbm, w_hbm, pieces_ref, out_ref, readout, weight, result, in_sems, out_sems):
    count, depth, width = weight.shape
    tokens = readout.shape[0]
    rows = tokens // out_sems.shape[1]
    me = lax.axis_index("head")

    def fetch(shift):
        if shift:
            source = pieces_ref.at[shift - 1]
        else:
            source = w_hbm.at[pl.ds(pl.multiple_of(me * depth, depth), depth)]
        return pltpu.make_async_copy(source, weight.at[shift], in_sems.at[shift])

    load = pltpu.make_async_copy(r_hbm, readout, in_sems.at[count])
    load.start()
    for shift in range(count):
        fetch(shift).start()
    load.wait()
    stores = []
    for shift in range(count):
        fetch(shift).wait()
        owner = lax.rem(me + count - shift, count)
        columns = pl.ds(pl.multiple_of(owner * width, width), width)
        for block in range(tokens // rows):
            part = pl.ds(block * rows, rows)
            result[shift, part] = dot(readout[part], weight[shift]).astype(result.dtype)
            stores.append(
                pltpu.make_async_copy(
                    result.at[shift, part], out_ref.at[0, part, columns], out_sems.at[shift, block]
                )
            )
            stores[-1].start()
    for store in stores:
        store.wait()


def shards(n_seq, n_head, queries, keys, values, gates, ridge, out_weight):
    tokens, head_width = queries.shape
    heads = head_width // HD
    half = heads // 2
    blocks = tokens // SPAN
    pairs = n_seq // 2
    width = out_weight.shape[1]
    tile = SPAN * HD * HD * 2
    hbm = pl.BlockSpec(memory_space=pl.ANY)
    in_vmem = pl.BlockSpec(memory_space=pltpu.VMEM)

    def square(*lead, dtype=f32):
        return pltpu.VMEM((*lead, HD, HD), dtype)

    every, some = heads * blocks, half * blocks
    readout, pieces = pl.pallas_call(
        functools.partial(solve_kernel, n_seq, n_head),
        in_specs=[hbm, hbm, hbm, in_vmem, pl.BlockSpec(memory_space=pltpu.SMEM), hbm],
        out_specs=[in_vmem, hbm],
        out_shape=[
            jax.ShapeDtypeStruct((tokens, head_width), bf16),
            jax.ShapeDtypeStruct((n_head - 1, 2, 4, head_width // 8, width), bf16),
        ],
        scratch_shapes=[
            *[pltpu.VMEM((tokens, head_width), bf16)] * 3,
            pltpu.VMEM((tokens, heads), f32),
            *[square(every, dtype=bf16)] * 3,
            *[square(every)] * 3,
            *[square(some, dtype=bf16)] * 2,
            *[square(some)] * 5,
            square(2, heads),
            square(2, half), square(half), square(half, dtype=bf16),
            square(pairs - 1, half), square(pairs - 1, half, dtype=bf16),
            square(2, half), square(2, 2, half),
            pltpu.SemaphoreType.DMA((3,)),
            pltpu.SemaphoreType.DMA((2, n_head - 1)),
            pltpu.SemaphoreType.DMA((2, 2)),
            pltpu.SemaphoreType.DMA((2, 2)),
            pltpu.SemaphoreType.DMA((2, 2)),
            pltpu.SemaphoreType.DMA((2, pairs - 1)),
            pltpu.SemaphoreType.DMA((2, pairs - 1)),
            pltpu.SemaphoreType.DMA((2, 2)),
        ],
        compiler_params=pltpu.CompilerParams(
            vmem_limit_bytes=VMEM_BYTES, collective_id=0, has_side_effects=True
        ),
        cost_estimate=pl.CostEstimate(
            flops=heads * blocks * 58 * tile, bytes_accessed=tokens * head_width * 8, transcendentals=0
        ),
        name="solve",
    )(keys, values, queries, gates.T, ridge, out_weight)
    return pl.pallas_call(
        project_kernel,
        in_specs=[hbm] * 3,
        out_specs=hbm,
        out_shape=jax.ShapeDtypeStruct((1, tokens, width * n_head), bf16),
        scratch_shapes=[
            pltpu.VMEM((tokens, head_width), bf16),
            pltpu.VMEM((n_head, head_width, width), bf16),
            pltpu.VMEM((n_head, tokens, width), bf16),
            pltpu.SemaphoreType.DMA((n_head + 1,)),
            pltpu.SemaphoreType.DMA((n_head, tokens // PROJECT_ROWS)),
        ],
        compiler_params=pltpu.CompilerParams(vmem_limit_bytes=VMEM_BYTES),
        cost_estimate=pl.CostEstimate(
            flops=2 * tokens * head_width * width * n_head,
            bytes_accessed=tokens * width * n_head * 2,
            transcendentals=0,
        ),
        name="project",
    )(readout, out_weight, pieces.reshape(n_head - 1, head_width, width))


def solution(mesh):
    return jax.shard_map(
        functools.partial(shards, mesh.shape["seq"], mesh.shape["head"]),
        mesh=mesh,
        in_specs=(
            P("seq", "head"),
            P("seq", "head"),
            P("seq", "head"),
            P("seq", "head"),
            P("head"),
            P(None, "head"),
        ),
        out_specs=P("head", "seq", None),
        check_vma=False,
    )
```

```python
import functools

import jax
import jax.numpy as jnp
from jax import lax
from jax.experimental import pallas as pl
from jax.experimental.pallas import tpu as pltpu
from jax.sharding import PartitionSpec as P

HD = 128
SPAN = 128
ITERS = 8
EPS = 1e-06
f32 = jnp.float32
bf16 = jnp.bfloat16
VMEM_BYTES = 56 * 1024 * 1024
MESH = pl.DeviceIdType.MESH
PROJECT_ROWS = 256


def dot(a, b):
    return jnp.dot(a, b, preferred_element_type=f32)


def two_terms(x):
    high = x.astype(bf16)
    return high, (x - high.astype(f32)).astype(bf16)


def row_sum(x):
    return jnp.sum(x, 1, keepdims=True)


def wide(x):
    return jnp.broadcast_to(x, (SPAN, HD))


def solve_kernel(
    n_seq, n_head,
    k_hbm, v_hbm, q_hbm, g_ref, ridge_ref, w_hbm, out_ref, pieces_ref,
    k_ref, v_ref, q_ref, gate_columns, keys_t, keys_w, values_w, scales, gram_local, moment_local,
    gram_high, gram_low, direct, res, sol, norms, images,
    own, mate, chip_gram, chip_moment, gram_slots, moment_slots, give, prior,
    load_sems, piece_sems, plane_sems, chip_sems, mate_sems, send_sems, recv_sems, back_sems,
):
    tokens, head_width = k_ref.shape
    heads = head_width // HD
    half = heads // 2
    blocks = tokens // SPAN
    pairs = n_seq // 2
    me = lax.axis_index("seq")
    group = lax.axis_index("head")
    side = lax.rem(me, 2)
    pair = me // 2
    mate_at = {"seq": me + 1 - 2 * side}
    mine = pl.ds(pl.multiple_of(side * (HD // 2), HD // 2), HD // 2)
    others = pl.ds(pl.multiple_of((1 - side) * (HD // 2), HD // 2), HD // 2)
    row = lax.broadcasted_iota(jnp.int32, (HD, HD), 0)
    col = lax.broadcasted_iota(jnp.int32, (HD, HD), 1)
    causal = (col <= row).astype(f32).astype(bf16)
    GRAM, MOMENT = 0, 1
    chip_sums, slots = (chip_gram, chip_moment), (gram_slots, moment_slots)

    loads = [
        pltpu.make_async_copy(src, dst, load_sems.at[i])
        for i, (src, dst) in enumerate(((k_hbm, k_ref), (v_hbm, v_ref), (q_hbm, q_ref)))
    ]
    for load in loads:
        load.start()

    barrier = pltpu.get_barrier_semaphore()
    pl.semaphore_signal(barrier, inc=1, device_id=mate_at, device_id_type=MESH)
    for off in range(1, pairs):
        target = {"seq": lax.rem(pair + off, pairs) * 2 + side}
        pl.semaphore_signal(barrier, inc=1, device_id=target, device_id_type=MESH)
    for shift in range(1, n_head):
        target = {"head": lax.rem(group + shift, n_head)}
        pl.semaphore_signal(barrier, inc=1, device_id=target, device_id_type=MESH)

    for c in range(blocks):
        rows = pl.ds(c * SPAN, SPAN)
        gate_columns[rows, :] = g_ref[:, rows].T

    def columns_of(h):
        return pl.ds(pl.multiple_of(h * HD, HD), HD)

    def sum_grams(first):
        def one(j, carry):
            h = first + j
            total = jnp.zeros((HD, HD), f32)
            for c in range(blocks):
                n = h * blocks + c
                rows = pl.ds(c * SPAN, SPAN)
                keys = k_ref[rows, columns_of(h)]
                keys_f = keys.astype(f32)
                s = lax.rsqrt(row_sum(keys_f * keys_f) + EPS)
                gates = gate_columns[rows, :]
                gate = row_sum(jnp.where(lax.broadcasted_iota(jnp.int32, gates.shape, 1) == h, gates, 0.0))
                w_value = gate * s
                high, low = two_terms(keys_f * (w_value * s))
                turned = keys.T
                keys_t[n] = turned
                keys_w[n] = high
                scales[n] = wide(w_value)
                gram_local[n] = total
                total += dot(jnp.concatenate([turned, turned], 1), jnp.concatenate([high, low], 0))
            own[GRAM, h] = total
            return carry

        lax.fori_loop(0, half, one, 0)

    def sum_moments(first):
        def one(j, carry):
            h = first + j
            total = jnp.zeros((HD, HD), f32)
            for c in range(blocks):
                n = h * blocks + c
                values = v_ref[pl.ds(c * SPAN, SPAN), columns_of(h)].astype(f32)
                high, low = two_terms(values * scales[n])
                values_w[n] = high
                moment_local[n] = total
                turned = keys_t[n]
                total += dot(jnp.concatenate([turned, turned], 1), jnp.concatenate([high, low], 0))
            own[MOMENT, h] = total
            return carry

        lax.fori_loop(0, half, one, 0)

    def heads_of(p):
        return pl.ds(p * half, half)

    def to_mate(kind, p):
        return pltpu.make_async_remote_copy(
            src_ref=own.at[kind, heads_of(p), others], dst_ref=mate.at[kind, p],
            send_sem=mate_sems.at[kind, p, 0], recv_sem=mate_sems.at[kind, p, 1],
            device_id=mate_at, device_id_type=MESH,
        )

    def to_later(kind, p, off):
        target = {"seq": lax.rem(pair + off, pairs) * 2 + side}
        return pltpu.make_async_remote_copy(
            src_ref=chip_sums[kind].at[p], dst_ref=slots[kind].at[p, off - 1],
            send_sem=send_sems.at[kind, p, off - 1], recv_sem=recv_sems.at[kind, p, off - 1],
            device_id=target, device_id_type=MESH,
        )

    def to_back(kind, p):
        return pltpu.make_async_remote_copy(
            src_ref=give.at[kind, p], dst_ref=prior.at[kind, heads_of(p), mine],
            send_sem=back_sems.at[kind, p, 0], recv_sem=back_sems.at[kind, p, 1],
            device_id=mate_at, device_id_type=MESH,
        )

    part = pieces_ref.shape[3]
    across = (pair + 1 - 2 * lax.rem(pair, 2), pair + 2 - 4 * lax.rem(pair // 2, 2))
    quarter = 2 * lax.rem(pair + pair // 2, 2)

    def to_head(shift):
        target = lax.rem(group + shift, n_head)
        start = pl.multiple_of(target * head_width + (side * 4 + quarter) * part, part)
        return pltpu.make_async_remote_copy(
            src_ref=w_hbm.at[pl.ds(start, 2 * part)].reshape(2, part, w_hbm.shape[1]),
            dst_ref=pieces_ref.at[shift - 1, side, pl.ds(quarter, 2)],
            send_sem=piece_sems.at[0, shift - 1], recv_sem=piece_sems.at[1, shift - 1],
            device_id={"head": target}, device_id_type=MESH,
        )

    def to_plane(i):
        shared = pieces_ref.at[:, side, quarter + i]
        return pltpu.make_async_remote_copy(
            src_ref=shared, dst_ref=shared,
            send_sem=plane_sems.at[0, i], recv_sem=plane_sems.at[1, i],
            device_id={"seq": across[i] * 2 + side}, device_id_type=MESH,
        )

    def to_chip(i):
        shared = pieces_ref.at[:, side, pl.ds(quarter + i * (2 - 2 * quarter), 2)]
        return pltpu.make_async_remote_copy(
            src_ref=shared, dst_ref=shared,
            send_sem=chip_sems.at[0, i], recv_sem=chip_sems.at[1, i],
            device_id=mate_at, device_id_type=MESH,
        )

    def pass_on(kind, p):
        to_mate(kind, p).wait_recv()
        chip = own[kind, heads_of(p), mine] + mate[kind, p]
        chip_sums[kind][p] = chip.astype(chip_sums[kind].dtype)
        for off in range(1, pairs):
            @pl.when(pair + off < pairs)
            def _():
                to_later(kind, p, off).start()

    def collect(kind, p):
        give[kind, p] = jnp.zeros((half, HD // 2, HD), f32)
        for off in range(1, pairs):
            @pl.when(pair >= off)
            def _():
                to_later(kind, p, off).wait_recv()
                give[kind, p] = give[kind, p] + slots[kind][p, off - 1].astype(f32)
        prior[kind, heads_of(p), mine] = give[kind, p] + side.astype(f32) * mate[kind, p]
        give[kind, p] = give[kind, p] + (1 - side).astype(f32) * own[kind, heads_of(p), mine]
        to_back(kind, p).start()

    def start_queries(p):
        def one(j, carry):
            for c in range(blocks):
                n = j * blocks + c
                queries = q_ref[pl.ds(c * SPAN, SPAN), columns_of(p * half + j)].astype(f32)
                square = row_sum(queries * queries)
                scale = lax.rsqrt(square + EPS)
                queries = queries * scale
                res[n] = queries
                direct[n] = queries
                norms[n] = wide(square * scale * scale)
            return carry

        lax.fori_loop(0, half, one, 0)

    loads[0].wait()
    sum_grams(0)
    pl.semaphore_wait(barrier, pairs + n_head - 1)
    to_mate(GRAM, 0).start()
    sum_grams(half)
    pass_on(GRAM, 0)
    to_mate(GRAM, 1).start()
    for shift in range(1, n_head):
        to_head(shift).start()
    loads[1].wait()
    sum_moments(0)
    to_mate(MOMENT, 0).start()
    loads[2].wait()
    start_queries(0)
    collect(GRAM, 0)
    sum_moments(half)
    to_mate(MOMENT, 1).start()
    to_back(GRAM, 0).wait_recv()

    def apply(n, at, d, high_ref, low_ref, right_ref, fine=True):
        half_right = jnp.concatenate([high_ref[n], keys_t[at]], 1)
        if fine:
            high, low = two_terms(d)
            first = dot(jnp.concatenate([high, low], 1), jnp.concatenate([half_right, half_right], 0))
        else:
            high = d.astype(bf16)
            first = dot(high, half_right)
        corr = first[:, HD:].astype(bf16) * causal
        if fine:
            left = jnp.concatenate([corr, high], 1)
            right = jnp.concatenate([right_ref[at], low_ref[n]], 0)
        else:
            left, right = corr, right_ref[at]
        second = dot(left, jnp.concatenate([right, right], 1))
        return first[:, :HD] + second[:, :HD]

    units = half * blocks
    behind = units // 2

    def run(p, carry):
        first = p * half

        @pl.when(p == 1)
        def _():
            start_queries(1)
            to_back(GRAM, 1).wait_recv()

        def split(kind, j, c, local):
            total = local[(first + j) * blocks + c] + prior[kind, first + j]
            if kind == GRAM:
                total += jnp.where(row == col, ridge_ref[first + j], 0.0)
            gram_high[j * blocks + c], gram_low[j * blocks + c] = two_terms(total)

        def prepare(j, carry):
            for c in range(blocks):
                split(GRAM, j, c, gram_local)
                sol[j * blocks + c] = jnp.zeros((SPAN, HD), f32)
            return carry

        lax.fori_loop(0, half, prepare, 0)

        def multiply(n, fine=True):
            images[n] = apply(n, first * blocks + n, direct[n], gram_high, gram_low, keys_w, fine)

        def update(n, last=False):
            d = direct[n]
            image = images[n]
            now = norms[n]
            step = now / (row_sum(d * image) + EPS)
            sol[n] = sol[n] + step * d
            if last:
                return
            r = res[n] - step * image
            res[n] = r
            following = wide(row_sum(r * r))
            norms[n] = following
            direct[n] = r + following / (now + EPS) * d

        def iteration(last=False, before_last=False):
            for n in range(behind):
                multiply(n, not last)
                update(behind + n, last)
            for n in range(behind):
                update(n, last)
                if not last:
                    multiply(behind + n, not before_last)

        for n in range(behind):
            multiply(behind + n)

        def sweep(i, carry):
            iteration()
            iteration()

            @pl.when((p == 0) & (i == 0))
            def _():
                pass_on(GRAM, 1)
                pass_on(MOMENT, 0)

            @pl.when((p == 0) & (i == 2))
            def _():
                pass_on(MOMENT, 1)

            @pl.when((p == 1) & (i == 2))
            def _():
                for which in range(2):
                    to_plane(which).wait_recv()
                to_chip(1).start()

            return carry

        lax.fori_loop(0, (ITERS - 2) // 2, sweep, 0)
        iteration(before_last=True)

        @pl.when(p == 0)
        def _():
            collect(MOMENT, 0)
            collect(GRAM, 1)

        @pl.when(p == 1)
        def _():
            collect(MOMENT, 1)

        iteration(last=True)

        @pl.when(p == 0)
        def _():
            for shift in range(1, n_head):
                to_head(shift).wait_recv()
            for which in range(2):
                to_plane(which).start()
            to_chip(0).start()

        to_back(MOMENT, p).wait_recv()

        def finish(j, carry):
            for c in range(blocks):
                split(MOMENT, j, c, moment_local)
            for c in range(blocks):
                n = j * blocks + c
                out_ref[pl.ds(c * SPAN, SPAN), columns_of(first + j)] = apply(
                    n, first * blocks + n, sol[n], gram_high, gram_low, values_w
                ).astype(out_ref.dtype)
            return carry

        lax.fori_loop(0, half, finish, 0)
        return carry

    lax.fori_loop(0, 2, run, 0)
    for kind in (GRAM, MOMENT):
        for p in range(2):
            to_mate(kind, p).wait_send()
            to_back(kind, p).wait_send()
            for off in range(1, pairs):
                @pl.when(pair + off < pairs)
                def _():
                    to_later(kind, p, off).wait_send()
    for shift in range(1, n_head):
        to_head(shift).wait_send()
    for i in range(2):
        to_plane(i).wait_send()
        to_chip(i).wait()


def project_kernel(r_hbm, w_hbm, pieces_ref, out_ref, readout, weight, result, in_sems, out_sems):
    count, depth, width = weight.shape
    tokens = readout.shape[0]
    rows = tokens // out_sems.shape[1]
    me = lax.axis_index("head")

    def fetch(shift):
        if shift:
            source = pieces_ref.at[shift - 1]
        else:
            source = w_hbm.at[pl.ds(pl.multiple_of(me * depth, depth), depth)]
        return pltpu.make_async_copy(source, weight.at[shift], in_sems.at[shift])

    load = pltpu.make_async_copy(r_hbm, readout, in_sems.at[count])
    load.start()
    for shift in range(count):
        fetch(shift).start()
    load.wait()
    stores = []
    for shift in range(count):
        fetch(shift).wait()
        owner = lax.rem(me + count - shift, count)
        columns = pl.ds(pl.multiple_of(owner * width, width), width)
        for block in range(tokens // rows):
            part = pl.ds(block * rows, rows)
            result[shift, part] = dot(readout[part], weight[shift]).astype(result.dtype)
            stores.append(
                pltpu.make_async_copy(
                    result.at[shift, part], out_ref.at[0, part, columns], out_sems.at[shift, block]
                )
            )
            stores[-1].start()
    for store in stores:
        store.wait()


def shards(n_seq, n_head, queries, keys, values, gates, ridge, out_weight):
    tokens, head_width = queries.shape
    heads = head_width // HD
    half = heads // 2
    blocks = tokens // SPAN
    pairs = n_seq // 2
    width = out_weight.shape[1]
    tile = SPAN * HD * HD * 2
    hbm = pl.BlockSpec(memory_space=pl.ANY)
    in_vmem = pl.BlockSpec(memory_space=pltpu.VMEM)

    def square(*lead, dtype=f32):
        return pltpu.VMEM((*lead, HD, HD), dtype)

    def strip(*lead, dtype=f32):
        return pltpu.VMEM((*lead, HD // 2, HD), dtype)

    every, some = heads * blocks, half * blocks
    readout, pieces = pl.pallas_call(
        functools.partial(solve_kernel, n_seq, n_head),
        in_specs=[hbm, hbm, hbm, in_vmem, pl.BlockSpec(memory_space=pltpu.SMEM), hbm],
        out_specs=[in_vmem, hbm],
        out_shape=[
            jax.ShapeDtypeStruct((tokens, head_width), bf16),
            jax.ShapeDtypeStruct((n_head - 1, 2, 4, head_width // 8, width), bf16),
        ],
        scratch_shapes=[
            *[pltpu.VMEM((tokens, head_width), bf16)] * 3,
            pltpu.VMEM((tokens, heads), f32),
            *[square(every, dtype=bf16)] * 3,
            *[square(every)] * 3,
            *[square(some, dtype=bf16)] * 2,
            *[square(some)] * 5,
            square(2, heads),
            strip(2, 2, half), strip(2, half), strip(2, half, dtype=bf16),
            strip(2, pairs - 1, half), strip(2, pairs - 1, half, dtype=bf16),
            strip(2, 2, half), square(2, heads),
            pltpu.SemaphoreType.DMA((3,)),
            pltpu.SemaphoreType.DMA((2, n_head - 1)),
            pltpu.SemaphoreType.DMA((2, 2)),
            pltpu.SemaphoreType.DMA((2, 2)),
            pltpu.SemaphoreType.DMA((2, 2, 2)),
            pltpu.SemaphoreType.DMA((2, 2, pairs - 1)),
            pltpu.SemaphoreType.DMA((2, 2, pairs - 1)),
            pltpu.SemaphoreType.DMA((2, 2, 2)),
        ],
        compiler_params=pltpu.CompilerParams(
            vmem_limit_bytes=VMEM_BYTES, collective_id=0, has_side_effects=True
        ),
        cost_estimate=pl.CostEstimate(
            flops=heads * blocks * 58 * tile, bytes_accessed=tokens * head_width * 8, transcendentals=0
        ),
        name="solve",
    )(keys, values, queries, gates.T, ridge, out_weight)
    return pl.pallas_call(
        project_kernel,
        in_specs=[hbm] * 3,
        out_specs=hbm,
        out_shape=jax.ShapeDtypeStruct((1, tokens, width * n_head), bf16),
        scratch_shapes=[
            pltpu.VMEM((tokens, head_width), bf16),
            pltpu.VMEM((n_head, head_width, width), bf16),
            pltpu.VMEM((n_head, tokens, width), bf16),
            pltpu.SemaphoreType.DMA((n_head + 1,)),
            pltpu.SemaphoreType.DMA((n_head, tokens // PROJECT_ROWS)),
        ],
        compiler_params=pltpu.CompilerParams(vmem_limit_bytes=VMEM_BYTES),
        cost_estimate=pl.CostEstimate(
            flops=2 * tokens * head_width * width * n_head,
            bytes_accessed=tokens * width * n_head * 2,
            transcendentals=0,
        ),
        name="project",
    )(readout, out_weight, pieces.reshape(n_head - 1, head_width, width))


def solution(mesh):
    return jax.shard_map(
        functools.partial(shards, mesh.shape["seq"], mesh.shape["head"]),
        mesh=mesh,
        in_specs=(
            P("seq", "head"),
            P("seq", "head"),
            P("seq", "head"),
            P("seq", "head"),
            P("head"),
            P(None, "head"),
        ),
        out_specs=P("head", "seq", None),
        check_vma=False,
    )
```

```python
import functools

import jax
import jax.numpy as jnp
from jax import lax
from jax.experimental import pallas as pl
from jax.experimental.pallas import tpu as pltpu
from jax.sharding import PartitionSpec as P

HD = 128
SPAN = 128
ITERS = 8
EPS = 1e-06
f32 = jnp.float32
bf16 = jnp.bfloat16
VMEM_BYTES = 56 * 1024 * 1024
PROJECT_BYTES = 16 * 1024 * 1024
MESH = pl.DeviceIdType.MESH
PROJECT_ROWS = 256


def dot(a, b):
    return jnp.dot(a, b, preferred_element_type=f32)


def two_terms(x):
    high = x.astype(bf16)
    return high, (x - high.astype(f32)).astype(bf16)


def row_sum(x):
    return jnp.sum(x, 1, keepdims=True)


def wide(x):
    return jnp.broadcast_to(x, (SPAN, HD))


def solve_kernel(
    n_seq, n_head,
    k_hbm, v_hbm, q_hbm, g_ref, ridge_ref, w_hbm, out_ref, pieces_ref,
    k_ref, v_ref, q_ref, gate_columns, keys_t, keys_w, values_w, scales, gram_local, moment_local,
    gram_high, gram_low, direct, res, sol, norms, images,
    own, mate, chip_gram, chip_moment, gram_slots, moment_slots, give, prior,
    load_sems, piece_sems, plane_sems, chip_sems, mate_sems, send_sems, recv_sems, back_sems,
):
    tokens, head_width = k_ref.shape
    heads = head_width // HD
    half = heads // 2
    blocks = tokens // SPAN
    pairs = n_seq // 2
    me = lax.axis_index("seq")
    group = lax.axis_index("head")
    side = lax.rem(me, 2)
    pair = me // 2
    mate_at = {"seq": me + 1 - 2 * side}
    mine = pl.ds(pl.multiple_of(side * (HD // 2), HD // 2), HD // 2)
    others = pl.ds(pl.multiple_of((1 - side) * (HD // 2), HD // 2), HD // 2)
    row = lax.broadcasted_iota(jnp.int32, (HD, HD), 0)
    col = lax.broadcasted_iota(jnp.int32, (HD, HD), 1)
    causal = (col <= row).astype(f32).astype(bf16)
    GRAM, MOMENT = 0, 1
    chip_sums, slots = (chip_gram, chip_moment), (gram_slots, moment_slots)

    loads = [
        pltpu.make_async_copy(src, dst, load_sems.at[i])
        for i, (src, dst) in enumerate(((k_hbm, k_ref), (v_hbm, v_ref), (q_hbm, q_ref)))
    ]
    for load in loads:
        load.start()

    barrier = pltpu.get_barrier_semaphore()
    pl.semaphore_signal(barrier, inc=1, device_id=mate_at, device_id_type=MESH)
    for off in range(1, pairs):
        target = {"seq": lax.rem(pair + off, pairs) * 2 + side}
        pl.semaphore_signal(barrier, inc=1, device_id=target, device_id_type=MESH)
    for shift in range(1, n_head):
        target = {"head": lax.rem(group + shift, n_head)}
        pl.semaphore_signal(barrier, inc=1, device_id=target, device_id_type=MESH)

    for c in range(blocks):
        rows = pl.ds(c * SPAN, SPAN)
        gate_columns[rows, :] = g_ref[:, rows].T

    def columns_of(h):
        return pl.ds(pl.multiple_of(h * HD, HD), HD)

    def sum_grams(first):
        def one(j, carry):
            h = first + j
            total = jnp.zeros((HD, HD), f32)
            for c in range(blocks):
                n = h * blocks + c
                rows = pl.ds(c * SPAN, SPAN)
                keys = k_ref[rows, columns_of(h)]
                keys_f = keys.astype(f32)
                s = lax.rsqrt(row_sum(keys_f * keys_f) + EPS)
                gates = gate_columns[rows, :]
                gate = row_sum(jnp.where(lax.broadcasted_iota(jnp.int32, gates.shape, 1) == h, gates, 0.0))
                w_value = gate * s
                high, low = two_terms(keys_f * (w_value * s))
                turned = keys.T
                keys_t[n] = turned
                keys_w[n] = high
                scales[n] = wide(w_value)
                gram_local[n] = total
                total += dot(jnp.concatenate([turned, turned], 1), jnp.concatenate([high, low], 0))
            own[GRAM, h] = total
            return carry

        lax.fori_loop(0, half, one, 0)

    def sum_moments(first):
        def one(j, carry):
            h = first + j
            total = jnp.zeros((HD, HD), f32)
            for c in range(blocks):
                n = h * blocks + c
                values = v_ref[pl.ds(c * SPAN, SPAN), columns_of(h)].astype(f32)
                high, low = two_terms(values * scales[n])
                values_w[n] = high
                moment_local[n] = total
                turned = keys_t[n]
                total += dot(jnp.concatenate([turned, turned], 1), jnp.concatenate([high, low], 0))
            own[MOMENT, h] = total
            return carry

        lax.fori_loop(0, half, one, 0)

    def heads_of(p):
        return pl.ds(p * half, half)

    def to_mate(kind, p):
        return pltpu.make_async_remote_copy(
            src_ref=own.at[kind, heads_of(p), others], dst_ref=mate.at[kind, p],
            send_sem=mate_sems.at[kind, p, 0], recv_sem=mate_sems.at[kind, p, 1],
            device_id=mate_at, device_id_type=MESH,
        )

    def to_later(kind, p, off):
        target = {"seq": lax.rem(pair + off, pairs) * 2 + side}
        return pltpu.make_async_remote_copy(
            src_ref=chip_sums[kind].at[p], dst_ref=slots[kind].at[p, off - 1],
            send_sem=send_sems.at[kind, p, off - 1], recv_sem=recv_sems.at[kind, p, off - 1],
            device_id=target, device_id_type=MESH,
        )

    def to_back(kind, p):
        return pltpu.make_async_remote_copy(
            src_ref=give.at[kind, p], dst_ref=prior.at[kind, heads_of(p), mine],
            send_sem=back_sems.at[kind, p, 0], recv_sem=back_sems.at[kind, p, 1],
            device_id=mate_at, device_id_type=MESH,
        )

    part = pieces_ref.shape[3]
    across = (pair + 1 - 2 * lax.rem(pair, 2), pair + 2 - 4 * lax.rem(pair // 2, 2))
    quarter = 2 * lax.rem(pair + pair // 2, 2)

    def to_head(shift):
        target = lax.rem(group + shift, n_head)
        start = pl.multiple_of(target * head_width + (side * 4 + quarter) * part, part)
        return pltpu.make_async_remote_copy(
            src_ref=w_hbm.at[pl.ds(start, 2 * part)].reshape(2, part, w_hbm.shape[1]),
            dst_ref=pieces_ref.at[shift - 1, side, pl.ds(quarter, 2)],
            send_sem=piece_sems.at[0, shift - 1], recv_sem=piece_sems.at[1, shift - 1],
            device_id={"head": target}, device_id_type=MESH,
        )

    def to_plane(i):
        shared = pieces_ref.at[:, side, quarter + i]
        return pltpu.make_async_remote_copy(
            src_ref=shared, dst_ref=shared,
            send_sem=plane_sems.at[0, i], recv_sem=plane_sems.at[1, i],
            device_id={"seq": across[i] * 2 + side}, device_id_type=MESH,
        )

    def to_chip(i):
        shared = pieces_ref.at[:, side, pl.ds(quarter + i * (2 - 2 * quarter), 2)]
        return pltpu.make_async_remote_copy(
            src_ref=shared, dst_ref=shared,
            send_sem=chip_sems.at[0, i], recv_sem=chip_sems.at[1, i],
            device_id=mate_at, device_id_type=MESH,
        )

    def pass_on(kind, p):
        to_mate(kind, p).wait_recv()
        chip = own[kind, heads_of(p), mine] + mate[kind, p]
        chip_sums[kind][p] = chip.astype(chip_sums[kind].dtype)
        for off in range(1, pairs):
            @pl.when(pair + off < pairs)
            def _():
                to_later(kind, p, off).start()

    def collect(kind, p):
        give[kind, p] = jnp.zeros((half, HD // 2, HD), f32)
        for off in range(1, pairs):
            @pl.when(pair >= off)
            def _():
                to_later(kind, p, off).wait_recv()
                give[kind, p] = give[kind, p] + slots[kind][p, off - 1].astype(f32)
        prior[kind, heads_of(p), mine] = give[kind, p] + side.astype(f32) * mate[kind, p]
        give[kind, p] = give[kind, p] + (1 - side).astype(f32) * own[kind, heads_of(p), mine]
        to_back(kind, p).start()

    def start_queries(p):
        def one(j, carry):
            for c in range(blocks):
                n = j * blocks + c
                queries = q_ref[pl.ds(c * SPAN, SPAN), columns_of(p * half + j)].astype(f32)
                square = row_sum(queries * queries)
                scale = lax.rsqrt(square + EPS)
                queries = queries * scale
                res[n] = queries
                direct[n] = queries
                norms[n] = wide(square * scale * scale)
            return carry

        lax.fori_loop(0, half, one, 0)

    loads[0].wait()
    sum_grams(0)
    pl.semaphore_wait(barrier, pairs + n_head - 1)
    to_mate(GRAM, 0).start()
    sum_grams(half)
    pass_on(GRAM, 0)
    to_mate(GRAM, 1).start()
    for shift in range(1, n_head):
        to_head(shift).start()
    loads[1].wait()
    sum_moments(0)
    to_mate(MOMENT, 0).start()
    loads[2].wait()
    start_queries(0)
    collect(GRAM, 0)
    sum_moments(half)
    to_mate(MOMENT, 1).start()
    to_back(GRAM, 0).wait_recv()

    def apply(n, at, d, high_ref, low_ref, right_ref, fine=True):
        half_right = jnp.concatenate([high_ref[n], keys_t[at]], 1)
        if fine:
            high, low = two_terms(d)
            first = dot(jnp.concatenate([high, low], 1), jnp.concatenate([half_right, half_right], 0))
        else:
            high = d.astype(bf16)
            first = dot(high, half_right)
        corr = first[:, HD:].astype(bf16) * causal
        if fine:
            left = jnp.concatenate([corr, high], 1)
            right = jnp.concatenate([right_ref[at], low_ref[n]], 0)
        else:
            left, right = corr, right_ref[at]
        second = dot(left, jnp.concatenate([right, right], 1))
        return first[:, :HD] + second[:, :HD]

    units = half * blocks
    behind = units // 2

    def run(p, carry):
        first = p * half

        @pl.when(p == 1)
        def _():
            start_queries(1)
            to_back(GRAM, 1).wait_recv()

        def split(kind, j, c, local):
            total = local[(first + j) * blocks + c] + prior[kind, first + j]
            if kind == GRAM:
                total += jnp.where(row == col, ridge_ref[first + j], 0.0)
            gram_high[j * blocks + c], gram_low[j * blocks + c] = two_terms(total)

        def prepare(j, carry):
            for c in range(blocks):
                split(GRAM, j, c, gram_local)
                sol[j * blocks + c] = jnp.zeros((SPAN, HD), f32)
            return carry

        lax.fori_loop(0, half, prepare, 0)

        def multiply(n, fine=True):
            images[n] = apply(n, first * blocks + n, direct[n], gram_high, gram_low, keys_w, fine)

        def update(n, last=False):
            d = direct[n]
            image = images[n]
            now = norms[n]
            step = now / (row_sum(d * image) + EPS)
            sol[n] = sol[n] + step * d
            if last:
                return
            r = res[n] - step * image
            res[n] = r
            following = wide(row_sum(r * r))
            norms[n] = following
            direct[n] = r + following / (now + EPS) * d

        def iteration(last=False, before_last=False):
            for n in range(behind):
                multiply(n, not last)
                update(behind + n, last)
            for n in range(behind):
                update(n, last)
                if not last:
                    multiply(behind + n, not before_last)

        for n in range(behind):
            multiply(behind + n)

        def sweep(i, carry):
            iteration()
            iteration()

            @pl.when((p == 0) & (i == 0))
            def _():
                pass_on(GRAM, 1)
                pass_on(MOMENT, 0)

            @pl.when((p == 0) & (i == 2))
            def _():
                pass_on(MOMENT, 1)

            @pl.when((p == 1) & (i == 2))
            def _():
                for which in range(2):
                    to_plane(which).wait_recv()
                to_chip(1).start()

            return carry

        lax.fori_loop(0, (ITERS - 2) // 2, sweep, 0)
        iteration(before_last=True)

        @pl.when(p == 0)
        def _():
            collect(MOMENT, 0)
            collect(GRAM, 1)

        @pl.when(p == 1)
        def _():
            collect(MOMENT, 1)

        iteration(last=True)

        @pl.when(p == 0)
        def _():
            for shift in range(1, n_head):
                to_head(shift).wait_recv()
            for which in range(2):
                to_plane(which).start()
            to_chip(0).start()

        to_back(MOMENT, p).wait_recv()

        def finish(j, carry):
            for c in range(blocks):
                split(MOMENT, j, c, moment_local)
            for c in range(blocks):
                n = j * blocks + c
                out_ref[pl.ds(c * SPAN, SPAN), columns_of(first + j)] = apply(
                    n, first * blocks + n, sol[n], gram_high, gram_low, values_w
                ).astype(out_ref.dtype)
            return carry

        lax.fori_loop(0, half, finish, 0)
        return carry

    lax.fori_loop(0, 2, run, 0)
    for kind in (GRAM, MOMENT):
        for p in range(2):
            to_mate(kind, p).wait_send()
            to_back(kind, p).wait_send()
            for off in range(1, pairs):
                @pl.when(pair + off < pairs)
                def _():
                    to_later(kind, p, off).wait_send()
    for shift in range(1, n_head):
        to_head(shift).wait_send()
    for i in range(2):
        to_plane(i).wait_send()
        to_chip(i).wait()


def project_kernel(readout, w_hbm, pieces_ref, out_ref, weight, result, in_sem, out_sems):
    count, tokens, width = result.shape
    depth = readout.shape[1]
    rows = tokens // out_sems.shape[1]
    me = lax.axis_index("head")
    own = w_hbm.at[pl.ds(pl.multiple_of(me * depth, depth), depth)]
    fetch = pltpu.make_async_copy(own, weight, in_sem)
    fetch.start()
    stores = []
    for shift in (*range(1, count), 0):
        if shift:
            piece = pieces_ref[shift - 1].reshape(depth, width)
        else:
            fetch.wait()
            piece = weight[...]
        owner = lax.rem(me + count - shift, count)
        columns = pl.ds(pl.multiple_of(owner * width, width), width)
        for block in range(tokens // rows):
            part = pl.ds(block * rows, rows)
            result[shift, part] = dot(readout[part], piece).astype(result.dtype)
            stores.append(
                pltpu.make_async_copy(
                    result.at[shift, part], out_ref.at[0, part, columns], out_sems.at[shift, block]
                )
            )
            stores[-1].start()
    for store in stores:
        store.wait()


def shards(n_seq, n_head, queries, keys, values, gates, ridge, out_weight):
    tokens, head_width = queries.shape
    heads = head_width // HD
    half = heads // 2
    blocks = tokens // SPAN
    pairs = n_seq // 2
    width = out_weight.shape[1]
    tile = SPAN * HD * HD * 2
    hbm = pl.BlockSpec(memory_space=pl.ANY)
    in_vmem = pl.BlockSpec(memory_space=pltpu.VMEM)

    def square(*lead, dtype=f32):
        return pltpu.VMEM((*lead, HD, HD), dtype)

    def strip(*lead, dtype=f32):
        return pltpu.VMEM((*lead, HD // 2, HD), dtype)

    every, some = heads * blocks, half * blocks
    readout, pieces = pl.pallas_call(
        functools.partial(solve_kernel, n_seq, n_head),
        in_specs=[hbm, hbm, hbm, in_vmem, pl.BlockSpec(memory_space=pltpu.SMEM), hbm],
        out_specs=[in_vmem, in_vmem],
        out_shape=[
            pltpu.VMEM((tokens, head_width), bf16),
            pltpu.VMEM((n_head - 1, 2, 4, head_width // 8, width), bf16),
        ],
        scratch_shapes=[
            *[pltpu.VMEM((tokens, head_width), bf16)] * 3,
            pltpu.VMEM((tokens, heads), f32),
            *[square(every, dtype=bf16)] * 3,
            *[square(every)] * 3,
            *[square(some, dtype=bf16)] * 2,
            *[square(some)] * 5,
            square(2, heads),
            strip(2, 2, half), strip(2, half), strip(2, half, dtype=bf16),
            strip(2, pairs - 1, half), strip(2, pairs - 1, half, dtype=bf16),
            strip(2, 2, half), square(2, heads),
            pltpu.SemaphoreType.DMA((3,)),
            pltpu.SemaphoreType.DMA((2, n_head - 1)),
            pltpu.SemaphoreType.DMA((2, 2)),
            pltpu.SemaphoreType.DMA((2, 2)),
            pltpu.SemaphoreType.DMA((2, 2, 2)),
            pltpu.SemaphoreType.DMA((2, 2, pairs - 1)),
            pltpu.SemaphoreType.DMA((2, 2, pairs - 1)),
            pltpu.SemaphoreType.DMA((2, 2, 2)),
        ],
        compiler_params=pltpu.CompilerParams(
            vmem_limit_bytes=VMEM_BYTES, collective_id=0, has_side_effects=True
        ),
        cost_estimate=pl.CostEstimate(
            flops=heads * blocks * 58 * tile, bytes_accessed=tokens * head_width * 8, transcendentals=0
        ),
        name="solve",
    )(keys, values, queries, gates.T, ridge, out_weight)
    return pl.pallas_call(
        project_kernel,
        in_specs=[in_vmem, hbm, in_vmem],
        out_specs=hbm,
        out_shape=jax.ShapeDtypeStruct((1, tokens, width * n_head), bf16),
        scratch_shapes=[
            pltpu.VMEM((head_width, width), bf16),
            pltpu.VMEM((n_head, tokens, width), bf16),
            pltpu.SemaphoreType.DMA(()),
            pltpu.SemaphoreType.DMA((n_head, tokens // PROJECT_ROWS)),
        ],
        compiler_params=pltpu.CompilerParams(vmem_limit_bytes=PROJECT_BYTES),
        cost_estimate=pl.CostEstimate(
            flops=2 * tokens * head_width * width * n_head,
            bytes_accessed=tokens * width * n_head * 2,
            transcendentals=0,
        ),
        name="project",
    )(readout, out_weight, pieces)


def solution(mesh):
    return jax.shard_map(
        functools.partial(shards, mesh.shape["seq"], mesh.shape["head"]),
        mesh=mesh,
        in_specs=(
            P("seq", "head"),
            P("seq", "head"),
            P("seq", "head"),
            P("seq", "head"),
            P("head"),
            P(None, "head"),
        ),
        out_specs=P("head", "seq", None),
        check_vma=False,
    )
```

```python
import functools

import jax
import jax.numpy as jnp
from jax import lax
from jax.experimental import pallas as pl
from jax.experimental.pallas import tpu as pltpu
from jax.sharding import PartitionSpec as P

HD = 128
SPAN = 128
ITERS = 8
EPS = 1e-06
f32 = jnp.float32
bf16 = jnp.bfloat16
VMEM_BYTES = 56 * 1024 * 1024
PROJECT_BYTES = 16 * 1024 * 1024
MESH = pl.DeviceIdType.MESH
PROJECT_ROWS = 256


def dot(a, b):
    return jnp.dot(a, b, preferred_element_type=f32)


def two_terms(x):
    high = x.astype(bf16)
    return high, (x - high.astype(f32)).astype(bf16)


def row_sum(x):
    return jnp.sum(x, 1, keepdims=True)


def wide(x):
    return jnp.broadcast_to(x, (SPAN, HD))


def solve_kernel(
    n_seq, n_head,
    k_hbm, v_hbm, q_hbm, g_ref, ridge_ref, w_hbm, out_ref, pieces_ref,
    k_ref, v_ref, q_ref, gate_columns, keys_t, keys_w, values_w, scales, gram_local, moment_local,
    gram_high, gram_low, direct, res, sol, norms, images,
    own, mate, chip_gram, chip_moment, gram_slots, moment_slots, give, prior,
    load_sems, piece_sems, plane_sems, chip_sems, mate_sems, send_sems, recv_sems, back_sems,
):
    tokens, head_width = k_ref.shape
    heads = head_width // HD
    half = heads // 2
    blocks = tokens // SPAN
    pairs = n_seq // 2
    me = lax.axis_index("seq")
    group = lax.axis_index("head")
    side = lax.rem(me, 2)
    pair = me // 2
    mate_at = {"seq": me + 1 - 2 * side}
    mine = pl.ds(pl.multiple_of(side * (HD // 2), HD // 2), HD // 2)
    others = pl.ds(pl.multiple_of((1 - side) * (HD // 2), HD // 2), HD // 2)
    row = lax.broadcasted_iota(jnp.int32, (HD, HD), 0)
    col = lax.broadcasted_iota(jnp.int32, (HD, HD), 1)
    causal = (col <= row).astype(f32).astype(bf16)
    GRAM, MOMENT = 0, 1
    chip_sums, slots = (chip_gram, chip_moment), (gram_slots, moment_slots)

    near, far = pl.ds(0, half * HD), pl.ds(half * HD, half * HD)
    loads = [
        pltpu.make_async_copy(src, dst, load_sems.at[i])
        for i, (src, dst) in enumerate((
            (k_hbm.at[:, near], k_ref.at[:, near]), (k_hbm.at[:, far], k_ref.at[:, far]),
            (v_hbm, v_ref), (q_hbm, q_ref),
        ))
    ]
    for load in loads:
        load.start()

    barrier = pltpu.get_barrier_semaphore()
    pl.semaphore_signal(barrier, inc=1, device_id=mate_at, device_id_type=MESH)
    for off in range(1, pairs):
        target = {"seq": lax.rem(pair + off, pairs) * 2 + side}
        pl.semaphore_signal(barrier, inc=1, device_id=target, device_id_type=MESH)
    for shift in range(1, n_head):
        target = {"head": lax.rem(group + shift, n_head)}
        pl.semaphore_signal(barrier, inc=1, device_id=target, device_id_type=MESH)

    for c in range(blocks):
        rows = pl.ds(c * SPAN, SPAN)
        gate_columns[rows, :] = g_ref[:, rows].T

    def columns_of(h):
        return pl.ds(pl.multiple_of(h * HD, HD), HD)

    def sum_grams(first):
        def one(j, carry):
            h = first + j
            total = jnp.zeros((HD, HD), f32)
            for c in range(blocks):
                n = h * blocks + c
                rows = pl.ds(c * SPAN, SPAN)
                keys = k_ref[rows, columns_of(h)]
                keys_f = keys.astype(f32)
                s = lax.rsqrt(row_sum(keys_f * keys_f) + EPS)
                gates = gate_columns[rows, :]
                gate = row_sum(jnp.where(lax.broadcasted_iota(jnp.int32, gates.shape, 1) == h, gates, 0.0))
                w_value = gate * s
                high, low = two_terms(keys_f * (w_value * s))
                turned = keys.T
                keys_t[n] = turned
                keys_w[n] = high
                scales[n] = wide(w_value)
                gram_local[n] = total
                total += dot(jnp.concatenate([turned, turned], 1), jnp.concatenate([high, low], 0))
            own[GRAM, h] = total
            return carry

        for j in range(half):
            one(j, 0)

    def sum_moments(first):
        def one(j, carry):
            h = first + j
            total = jnp.zeros((HD, HD), f32)
            for c in range(blocks):
                n = h * blocks + c
                values = v_ref[pl.ds(c * SPAN, SPAN), columns_of(h)].astype(f32)
                high, low = two_terms(values * scales[n])
                values_w[n] = high
                moment_local[n] = total
                turned = keys_t[n]
                total += dot(jnp.concatenate([turned, turned], 1), jnp.concatenate([high, low], 0))
            own[MOMENT, h] = total
            return carry

        for j in range(half):
            one(j, 0)

    def heads_of(p):
        return pl.ds(p * half, half)

    def to_mate(kind, p):
        return pltpu.make_async_remote_copy(
            src_ref=own.at[kind, heads_of(p), others], dst_ref=mate.at[kind, p],
            send_sem=mate_sems.at[kind, p, 0], recv_sem=mate_sems.at[kind, p, 1],
            device_id=mate_at, device_id_type=MESH,
        )

    def to_later(kind, p, off):
        target = {"seq": lax.rem(pair + off, pairs) * 2 + side}
        return pltpu.make_async_remote_copy(
            src_ref=chip_sums[kind].at[p], dst_ref=slots[kind].at[p, off - 1],
            send_sem=send_sems.at[kind, p, off - 1], recv_sem=recv_sems.at[kind, p, off - 1],
            device_id=target, device_id_type=MESH,
        )

    def to_back(kind, p):
        return pltpu.make_async_remote_copy(
            src_ref=give.at[kind, p], dst_ref=prior.at[kind, heads_of(p), mine],
            send_sem=back_sems.at[kind, p, 0], recv_sem=back_sems.at[kind, p, 1],
            device_id=mate_at, device_id_type=MESH,
        )

    part = pieces_ref.shape[3]
    across = (pair + 1 - 2 * lax.rem(pair, 2), pair + 2 - 4 * lax.rem(pair // 2, 2))
    quarter = 2 * lax.rem(pair + pair // 2, 2)

    def to_head(shift):
        target = lax.rem(group + shift, n_head)
        start = pl.multiple_of(target * head_width + (side * 4 + quarter) * part, part)
        return pltpu.make_async_remote_copy(
            src_ref=w_hbm.at[pl.ds(start, 2 * part)].reshape(2, part, w_hbm.shape[1]),
            dst_ref=pieces_ref.at[shift - 1, side, pl.ds(quarter, 2)],
            send_sem=piece_sems.at[0, shift - 1], recv_sem=piece_sems.at[1, shift - 1],
            device_id={"head": target}, device_id_type=MESH,
        )

    def to_plane(i):
        shared = pieces_ref.at[:, side, quarter + i]
        return pltpu.make_async_remote_copy(
            src_ref=shared, dst_ref=shared,
            send_sem=plane_sems.at[0, i], recv_sem=plane_sems.at[1, i],
            device_id={"seq": across[i] * 2 + side}, device_id_type=MESH,
        )

    def to_chip(i):
        shared = pieces_ref.at[:, side, pl.ds(quarter + i * (2 - 2 * quarter), 2)]
        return pltpu.make_async_remote_copy(
            src_ref=shared, dst_ref=shared,
            send_sem=chip_sems.at[0, i], recv_sem=chip_sems.at[1, i],
            device_id=mate_at, device_id_type=MESH,
        )

    def pass_on(kind, p):
        to_mate(kind, p).wait_recv()
        chip = own[kind, heads_of(p), mine] + mate[kind, p]
        chip_sums[kind][p] = chip.astype(chip_sums[kind].dtype)
        for off in range(1, pairs):
            @pl.when(pair + off < pairs)
            def _():
                to_later(kind, p, off).start()

    def collect(kind, p):
        give[kind, p] = jnp.zeros((half, HD // 2, HD), f32)
        for off in range(1, pairs):
            @pl.when(pair >= off)
            def _():
                to_later(kind, p, off).wait_recv()
                give[kind, p] = give[kind, p] + slots[kind][p, off - 1].astype(f32)
        prior[kind, heads_of(p), mine] = give[kind, p] + side.astype(f32) * mate[kind, p]
        give[kind, p] = give[kind, p] + (1 - side).astype(f32) * own[kind, heads_of(p), mine]
        to_back(kind, p).start()

    def start_queries(p):
        def one(j, carry):
            for c in range(blocks):
                n = j * blocks + c
                queries = q_ref[pl.ds(c * SPAN, SPAN), columns_of(p * half + j)].astype(f32)
                square = row_sum(queries * queries)
                scale = lax.rsqrt(square + EPS)
                queries = queries * scale
                res[n] = queries
                direct[n] = queries
                norms[n] = wide(square * scale * scale)
            return carry

        for j in range(half):
            one(j, 0)

    loads[0].wait()
    sum_grams(0)
    pl.semaphore_wait(barrier, pairs + n_head - 1)
    to_mate(GRAM, 0).start()
    loads[1].wait()
    sum_grams(half)
    pass_on(GRAM, 0)
    to_mate(GRAM, 1).start()
    for shift in range(1, n_head):
        to_head(shift).start()
    loads[2].wait()
    sum_moments(0)
    to_mate(MOMENT, 0).start()
    loads[3].wait()
    start_queries(0)
    collect(GRAM, 0)
    sum_moments(half)
    to_mate(MOMENT, 1).start()
    to_back(GRAM, 0).wait_recv()

    def apply(n, at, d, high_ref, low_ref, right_ref, fine=True):
        half_right = jnp.concatenate([high_ref[n], keys_t[at]], 1)
        if fine:
            high, low = two_terms(d)
            first = dot(jnp.concatenate([high, low], 1), jnp.concatenate([half_right, half_right], 0))
        else:
            high = d.astype(bf16)
            first = dot(high, half_right)
        corr = first[:, HD:].astype(bf16) * causal
        if fine:
            left = jnp.concatenate([corr, high], 1)
            right = jnp.concatenate([right_ref[at], low_ref[n]], 0)
        else:
            left, right = corr, right_ref[at]
        second = dot(left, jnp.concatenate([right, right], 1))
        return first[:, :HD] + second[:, :HD]

    units = half * blocks
    behind = units // 2

    def run(p, carry):
        first = p * half

        @pl.when(p == 1)
        def _():
            start_queries(1)
            to_back(GRAM, 1).wait_recv()

        def split(kind, j, c, local):
            total = local[(first + j) * blocks + c] + prior[kind, first + j]
            if kind == GRAM:
                total += jnp.where(row == col, ridge_ref[first + j], 0.0)
            gram_high[j * blocks + c], gram_low[j * blocks + c] = two_terms(total)

        def prepare(j, carry):
            for c in range(blocks):
                split(GRAM, j, c, gram_local)
                sol[j * blocks + c] = jnp.zeros((SPAN, HD), f32)
            return carry

        for j in range(half):
            prepare(j, 0)

        def multiply(n, fine=True):
            images[n] = apply(n, first * blocks + n, direct[n], gram_high, gram_low, keys_w, fine)

        def update(n, last=False):
            d = direct[n]
            image = images[n]
            now = norms[n]
            step = now / (row_sum(d * image) + EPS)
            sol[n] = sol[n] + step * d
            if last:
                return
            r = res[n] - step * image
            res[n] = r
            following = wide(row_sum(r * r))
            norms[n] = following
            direct[n] = r + following / (now + EPS) * d

        def iteration(last=False, before_last=False):
            for n in range(behind):
                multiply(n, not last)
                update(behind + n, last)
            for n in range(behind):
                update(n, last)
                if not last:
                    multiply(behind + n, not before_last)

        for n in range(behind):
            multiply(behind + n)

        def sweep(i, carry):
            iteration()
            iteration()

            @pl.when((p == 0) & (i == 0))
            def _():
                pass_on(GRAM, 1)
                pass_on(MOMENT, 0)

            @pl.when((p == 0) & (i == 2))
            def _():
                pass_on(MOMENT, 1)

            @pl.when((p == 1) & (i == 2))
            def _():
                for which in range(2):
                    to_plane(which).wait_recv()
                to_chip(1).start()

            return carry

        lax.fori_loop(0, (ITERS - 2) // 2, sweep, 0)
        iteration(before_last=True)

        @pl.when(p == 0)
        def _():
            collect(MOMENT, 0)
            collect(GRAM, 1)

        @pl.when(p == 1)
        def _():
            collect(MOMENT, 1)

        iteration(last=True)

        @pl.when(p == 0)
        def _():
            for shift in range(1, n_head):
                to_head(shift).wait_recv()
            for which in range(2):
                to_plane(which).start()
            to_chip(0).start()

        to_back(MOMENT, p).wait_recv()

        def finish(j, carry):
            for c in range(blocks):
                split(MOMENT, j, c, moment_local)
            for c in range(blocks):
                n = j * blocks + c
                out_ref[pl.ds(c * SPAN, SPAN), columns_of(first + j)] = apply(
                    n, first * blocks + n, sol[n], gram_high, gram_low, values_w
                ).astype(out_ref.dtype)
            return carry

        for j in range(half):
            finish(j, 0)
        return carry

    lax.fori_loop(0, 2, run, 0)
    for kind in (GRAM, MOMENT):
        for p in range(2):
            to_mate(kind, p).wait_send()
            to_back(kind, p).wait_send()
            for off in range(1, pairs):
                @pl.when(pair + off < pairs)
                def _():
                    to_later(kind, p, off).wait_send()
    for shift in range(1, n_head):
        to_head(shift).wait_send()
    for i in range(2):
        to_plane(i).wait_send()
        to_chip(i).wait()


def project_kernel(readout, w_hbm, pieces_ref, out_ref, weight, result, in_sem, out_sems):
    count, tokens, width = result.shape
    depth = readout.shape[1]
    rows = tokens // out_sems.shape[1]
    me = lax.axis_index("head")
    own = w_hbm.at[pl.ds(pl.multiple_of(me * depth, depth), depth)]
    fetch = pltpu.make_async_copy(own, weight, in_sem)
    fetch.start()
    stores = []
    for shift in (*range(1, count), 0):
        if shift:
            piece = pieces_ref[shift - 1].reshape(depth, width)
        else:
            fetch.wait()
            piece = weight[...]
        owner = lax.rem(me + count - shift, count)
        columns = pl.ds(pl.multiple_of(owner * width, width), width)
        for block in range(tokens // rows):
            part = pl.ds(block * rows, rows)
            result[shift, part] = dot(readout[part], piece).astype(result.dtype)
            stores.append(
                pltpu.make_async_copy(
                    result.at[shift, part], out_ref.at[0, part, columns], out_sems.at[shift, block]
                )
            )
            stores[-1].start()
    for store in stores:
        store.wait()


def shards(n_seq, n_head, queries, keys, values, gates, ridge, out_weight):
    tokens, head_width = queries.shape
    heads = head_width // HD
    half = heads // 2
    blocks = tokens // SPAN
    pairs = n_seq // 2
    width = out_weight.shape[1]
    tile = SPAN * HD * HD * 2
    hbm = pl.BlockSpec(memory_space=pl.ANY)
    in_vmem = pl.BlockSpec(memory_space=pltpu.VMEM)

    def square(*lead, dtype=f32):
        return pltpu.VMEM((*lead, HD, HD), dtype)

    def strip(*lead, dtype=f32):
        return pltpu.VMEM((*lead, HD // 2, HD), dtype)

    every, some = heads * blocks, half * blocks
    readout, pieces = pl.pallas_call(
        functools.partial(solve_kernel, n_seq, n_head),
        in_specs=[hbm, hbm, hbm, in_vmem, pl.BlockSpec(memory_space=pltpu.SMEM), hbm],
        out_specs=[in_vmem, in_vmem],
        out_shape=[
            pltpu.VMEM((tokens, head_width), bf16),
            pltpu.VMEM((n_head - 1, 2, 4, head_width // 8, width), bf16),
        ],
        scratch_shapes=[
            *[pltpu.VMEM((tokens, head_width), bf16)] * 3,
            pltpu.VMEM((tokens, heads), f32),
            *[square(every, dtype=bf16)] * 3,
            *[square(every)] * 3,
            *[square(some, dtype=bf16)] * 2,
            *[square(some)] * 5,
            square(2, heads),
            strip(2, 2, half), strip(2, half), strip(2, half, dtype=bf16),
            strip(2, pairs - 1, half), strip(2, pairs - 1, half, dtype=bf16),
            strip(2, 2, half), square(2, heads),
            pltpu.SemaphoreType.DMA((4,)),
            pltpu.SemaphoreType.DMA((2, n_head - 1)),
            pltpu.SemaphoreType.DMA((2, 2)),
            pltpu.SemaphoreType.DMA((2, 2)),
            pltpu.SemaphoreType.DMA((2, 2, 2)),
            pltpu.SemaphoreType.DMA((2, 2, pairs - 1)),
            pltpu.SemaphoreType.DMA((2, 2, pairs - 1)),
            pltpu.SemaphoreType.DMA((2, 2, 2)),
        ],
        compiler_params=pltpu.CompilerParams(
            vmem_limit_bytes=VMEM_BYTES, collective_id=0, has_side_effects=True
        ),
        cost_estimate=pl.CostEstimate(
            flops=heads * blocks * 58 * tile, bytes_accessed=tokens * head_width * 8, transcendentals=0
        ),
        name="solve",
    )(keys, values, queries, gates.T, ridge, out_weight)
    return pl.pallas_call(
        project_kernel,
        in_specs=[in_vmem, hbm, in_vmem],
        out_specs=hbm,
        out_shape=jax.ShapeDtypeStruct((1, tokens, width * n_head), bf16),
        scratch_shapes=[
            pltpu.VMEM((head_width, width), bf16),
            pltpu.VMEM((n_head, tokens, width), bf16),
            pltpu.SemaphoreType.DMA(()),
            pltpu.SemaphoreType.DMA((n_head, tokens // PROJECT_ROWS)),
        ],
        compiler_params=pltpu.CompilerParams(vmem_limit_bytes=PROJECT_BYTES),
        cost_estimate=pl.CostEstimate(
            flops=2 * tokens * head_width * width * n_head,
            bytes_accessed=tokens * width * n_head * 2,
            transcendentals=0,
        ),
        name="project",
    )(readout, out_weight, pieces)


def solution(mesh):
    return jax.shard_map(
        functools.partial(shards, mesh.shape["seq"], mesh.shape["head"]),
        mesh=mesh,
        in_specs=(
            P("seq", "head"),
            P("seq", "head"),
            P("seq", "head"),
            P("seq", "head"),
            P("head"),
            P(None, "head"),
        ),
        out_specs=P("head", "seq", None),
        check_vma=False,
    )
```

```python
import functools

import jax
import jax.numpy as jnp
from jax import lax
from jax.experimental import pallas as pl
from jax.experimental.pallas import tpu as pltpu
from jax.sharding import PartitionSpec as P

HD = 128
SPAN = 128
ITERS = 8
EPS = 1e-06
f32 = jnp.float32
bf16 = jnp.bfloat16
VMEM_BYTES = 56 * 1024 * 1024
PROJECT_BYTES = 16 * 1024 * 1024
MESH = pl.DeviceIdType.MESH
PROJECT_ROWS = 256


def dot(a, b):
    return jnp.dot(a, b, preferred_element_type=f32)


def two_terms(x):
    high = x.astype(bf16)
    return high, (x - high.astype(f32)).astype(bf16)


def row_sum(x):
    return jnp.sum(x, 1, keepdims=True)


def wide(x):
    return jnp.broadcast_to(x, (SPAN, HD))


def solve_kernel(
    n_seq, n_head,
    k_hbm, v_hbm, q_hbm, g_ref, ridge_ref, w_hbm, out_ref, pieces_ref,
    k_ref, v_ref, q_ref, gate_columns, keys_t, keys_w, values_w, scales, gram_local, moment_local,
    gram_high, gram_low, direct, res, sol, norms, images,
    own, mate, chip_gram, chip_moment, gram_slots, moment_slots, give, prior,
    load_sems, piece_sems, plane_sems, chip_sems, mate_sems, send_sems, recv_sems, back_sems,
):
    tokens, head_width = k_ref.shape
    heads = head_width // HD
    half = heads // 2
    blocks = tokens // SPAN
    pairs = n_seq // 2
    me = lax.axis_index("seq")
    group = lax.axis_index("head")
    side = lax.rem(me, 2)
    pair = me // 2
    mate_at = {"seq": me + 1 - 2 * side}
    mine = pl.ds(pl.multiple_of(side * (HD // 2), HD // 2), HD // 2)
    others = pl.ds(pl.multiple_of((1 - side) * (HD // 2), HD // 2), HD // 2)
    row = lax.broadcasted_iota(jnp.int32, (HD, HD), 0)
    col = lax.broadcasted_iota(jnp.int32, (HD, HD), 1)
    causal = (col <= row).astype(f32).astype(bf16)
    GRAM, MOMENT = 0, 1
    chip_sums, slots = (chip_gram, chip_moment), (gram_slots, moment_slots)

    near, far = pl.ds(0, half * HD), pl.ds(half * HD, half * HD)
    loads = [
        pltpu.make_async_copy(src, dst, load_sems.at[i])
        for i, (src, dst) in enumerate((
            (k_hbm.at[:, near], k_ref.at[:, near]), (k_hbm.at[:, far], k_ref.at[:, far]),
            (v_hbm, v_ref), (q_hbm, q_ref),
        ))
    ]
    loads[0].start()

    barrier = pltpu.get_barrier_semaphore()
    pl.semaphore_signal(barrier, inc=1, device_id=mate_at, device_id_type=MESH)
    for off in range(1, pairs):
        target = {"seq": lax.rem(pair + off, pairs) * 2 + side}
        pl.semaphore_signal(barrier, inc=1, device_id=target, device_id_type=MESH)
    for shift in range(1, n_head):
        target = {"head": lax.rem(group + shift, n_head)}
        pl.semaphore_signal(barrier, inc=1, device_id=target, device_id_type=MESH)

    for c in range(blocks):
        rows = pl.ds(c * SPAN, SPAN)
        gate_columns[rows, :] = g_ref[:, rows].T

    def columns_of(h):
        return pl.ds(pl.multiple_of(h * HD, HD), HD)

    def sum_grams(first):
        def one(j, carry):
            h = first + j
            total = jnp.zeros((HD, HD), f32)
            for c in range(blocks):
                n = h * blocks + c
                rows = pl.ds(c * SPAN, SPAN)
                keys = k_ref[rows, columns_of(h)]
                keys_f = keys.astype(f32)
                s = lax.rsqrt(row_sum(keys_f * keys_f) + EPS)
                gates = gate_columns[rows, :]
                gate = row_sum(jnp.where(lax.broadcasted_iota(jnp.int32, gates.shape, 1) == h, gates, 0.0))
                w_value = gate * s
                high, low = two_terms(keys_f * (w_value * s))
                turned = keys.T
                keys_t[n] = turned
                keys_w[n] = high
                scales[n] = wide(w_value)
                gram_local[n] = total
                total += dot(jnp.concatenate([turned, turned], 1), jnp.concatenate([high, low], 0))
            own[GRAM, h] = total
            return carry

        for j in range(half):
            one(j, 0)

    def sum_moments(first):
        def one(j, carry):
            h = first + j
            total = jnp.zeros((HD, HD), f32)
            for c in range(blocks):
                n = h * blocks + c
                values = v_ref[pl.ds(c * SPAN, SPAN), columns_of(h)].astype(f32)
                high, low = two_terms(values * scales[n])
                values_w[n] = high
                moment_local[n] = total
                turned = keys_t[n]
                total += dot(jnp.concatenate([turned, turned], 1), jnp.concatenate([high, low], 0))
            own[MOMENT, h] = total
            return carry

        for j in range(half):
            one(j, 0)

    def heads_of(p):
        return pl.ds(p * half, half)

    def to_mate(kind, p):
        return pltpu.make_async_remote_copy(
            src_ref=own.at[kind, heads_of(p), others], dst_ref=mate.at[kind, p],
            send_sem=mate_sems.at[kind, p, 0], recv_sem=mate_sems.at[kind, p, 1],
            device_id=mate_at, device_id_type=MESH,
        )

    def to_later(kind, p, off):
        target = {"seq": lax.rem(pair + off, pairs) * 2 + side}
        return pltpu.make_async_remote_copy(
            src_ref=chip_sums[kind].at[p], dst_ref=slots[kind].at[p, off - 1],
            send_sem=send_sems.at[kind, p, off - 1], recv_sem=recv_sems.at[kind, p, off - 1],
            device_id=target, device_id_type=MESH,
        )

    def to_back(kind, p):
        return pltpu.make_async_remote_copy(
            src_ref=give.at[kind, p], dst_ref=prior.at[kind, heads_of(p), mine],
            send_sem=back_sems.at[kind, p, 0], recv_sem=back_sems.at[kind, p, 1],
            device_id=mate_at, device_id_type=MESH,
        )

    part = pieces_ref.shape[3]
    across = (pair + 1 - 2 * lax.rem(pair, 2), pair + 2 - 4 * lax.rem(pair // 2, 2))
    quarter = 2 * lax.rem(pair + pair // 2, 2)

    def to_head(shift):
        target = lax.rem(group + shift, n_head)
        start = pl.multiple_of(target * head_width + (side * 4 + quarter) * part, part)
        return pltpu.make_async_remote_copy(
            src_ref=w_hbm.at[pl.ds(start, 2 * part)].reshape(2, part, w_hbm.shape[1]),
            dst_ref=pieces_ref.at[shift - 1, side, pl.ds(quarter, 2)],
            send_sem=piece_sems.at[0, shift - 1], recv_sem=piece_sems.at[1, shift - 1],
            device_id={"head": target}, device_id_type=MESH,
        )

    def to_plane(i):
        shared = pieces_ref.at[:, side, quarter + i]
        return pltpu.make_async_remote_copy(
            src_ref=shared, dst_ref=shared,
            send_sem=plane_sems.at[0, i], recv_sem=plane_sems.at[1, i],
            device_id={"seq": across[i] * 2 + side}, device_id_type=MESH,
        )

    def to_chip(i):
        shared = pieces_ref.at[:, side, pl.ds(quarter + i * (2 - 2 * quarter), 2)]
        return pltpu.make_async_remote_copy(
            src_ref=shared, dst_ref=shared,
            send_sem=chip_sems.at[0, i], recv_sem=chip_sems.at[1, i],
            device_id=mate_at, device_id_type=MESH,
        )

    def pass_on(kind, p):
        to_mate(kind, p).wait_recv()
        chip = own[kind, heads_of(p), mine] + mate[kind, p]
        chip_sums[kind][p] = chip.astype(chip_sums[kind].dtype)
        for off in range(1, pairs):
            @pl.when(pair + off < pairs)
            def _():
                to_later(kind, p, off).start()

    def collect(kind, p):
        give[kind, p] = jnp.zeros((half, HD // 2, HD), f32)
        for off in range(1, pairs):
            @pl.when(pair >= off)
            def _():
                to_later(kind, p, off).wait_recv()
                give[kind, p] = give[kind, p] + slots[kind][p, off - 1].astype(f32)
        prior[kind, heads_of(p), mine] = give[kind, p] + side.astype(f32) * mate[kind, p]
        give[kind, p] = give[kind, p] + (1 - side).astype(f32) * own[kind, heads_of(p), mine]
        to_back(kind, p).start()

    def start_queries(p):
        def one(j, carry):
            for c in range(blocks):
                n = j * blocks + c
                queries = q_ref[pl.ds(c * SPAN, SPAN), columns_of(p * half + j)].astype(f32)
                square = row_sum(queries * queries)
                scale = lax.rsqrt(square + EPS)
                queries = queries * scale
                res[n] = queries
                direct[n] = queries
                norms[n] = wide(square * scale * scale)
            return carry

        for j in range(half):
            one(j, 0)

    loads[0].wait()
    for load in loads[1:]:
        load.start()
    sum_grams(0)
    pl.semaphore_wait(barrier, pairs + n_head - 1)
    to_mate(GRAM, 0).start()
    loads[1].wait()
    sum_grams(half)
    pass_on(GRAM, 0)
    to_mate(GRAM, 1).start()
    for shift in range(1, n_head):
        to_head(shift).start()
    loads[2].wait()
    sum_moments(0)
    to_mate(MOMENT, 0).start()
    loads[3].wait()
    start_queries(0)
    collect(GRAM, 0)
    sum_moments(half)
    to_mate(MOMENT, 1).start()
    to_back(GRAM, 0).wait_recv()

    def apply(n, at, d, high_ref, low_ref, right_ref, fine=True):
        half_right = jnp.concatenate([high_ref[n], keys_t[at]], 1)
        if fine:
            high, low = two_terms(d)
            first = dot(jnp.concatenate([high, low], 1), jnp.concatenate([half_right, half_right], 0))
        else:
            high = d.astype(bf16)
            first = dot(high, half_right)
        corr = first[:, HD:].astype(bf16) * causal
        if fine:
            left = jnp.concatenate([corr, high], 1)
            right = jnp.concatenate([right_ref[at], low_ref[n]], 0)
        else:
            left, right = corr, right_ref[at]
        second = dot(left, jnp.concatenate([right, right], 1))
        return first[:, :HD] + second[:, :HD]

    units = half * blocks
    behind = units // 2

    def run(p, carry):
        first = p * half

        @pl.when(p == 1)
        def _():
            start_queries(1)
            to_back(GRAM, 1).wait_recv()

        def split(kind, j, c, local):
            total = local[(first + j) * blocks + c] + prior[kind, first + j]
            if kind == GRAM:
                total += jnp.where(row == col, ridge_ref[first + j], 0.0)
            gram_high[j * blocks + c], gram_low[j * blocks + c] = two_terms(total)

        def prepare(j, carry):
            for c in range(blocks):
                split(GRAM, j, c, gram_local)
                sol[j * blocks + c] = jnp.zeros((SPAN, HD), f32)
            return carry

        for j in range(half):
            prepare(j, 0)

        def multiply(n, fine=True):
            images[n] = apply(n, first * blocks + n, direct[n], gram_high, gram_low, keys_w, fine)

        def update(n, last=False):
            d = direct[n]
            image = images[n]
            now = norms[n]
            step = now / (row_sum(d * image) + EPS)
            sol[n] = sol[n] + step * d
            if last:
                return
            r = res[n] - step * image
            res[n] = r
            following = wide(row_sum(r * r))
            norms[n] = following
            direct[n] = r + following / (now + EPS) * d

        def iteration(last=False, before_last=False):
            for n in range(behind):
                multiply(n, not last)
                update(behind + n, last)
            for n in range(behind):
                update(n, last)
                if not last:
                    multiply(behind + n, not before_last)

        for n in range(behind):
            multiply(behind + n)

        def sweep(i, carry):
            iteration()
            iteration()

            @pl.when((p == 0) & (i == 0))
            def _():
                pass_on(GRAM, 1)
                pass_on(MOMENT, 0)

            @pl.when((p == 0) & (i == 2))
            def _():
                pass_on(MOMENT, 1)

            @pl.when((p == 1) & (i == 2))
            def _():
                for which in range(2):
                    to_plane(which).wait_recv()
                to_chip(1).start()

            return carry

        lax.fori_loop(0, (ITERS - 2) // 2, sweep, 0)
        iteration(before_last=True)

        @pl.when(p == 0)
        def _():
            collect(MOMENT, 0)
            collect(GRAM, 1)

        @pl.when(p == 1)
        def _():
            collect(MOMENT, 1)

        iteration(last=True)

        @pl.when(p == 0)
        def _():
            for shift in range(1, n_head):
                to_head(shift).wait_recv()
            for which in range(2):
                to_plane(which).start()
            to_chip(0).start()

        to_back(MOMENT, p).wait_recv()

        def finish(j, carry):
            for c in range(blocks):
                split(MOMENT, j, c, moment_local)
            for c in range(blocks):
                n = j * blocks + c
                out_ref[pl.ds(c * SPAN, SPAN), columns_of(first + j)] = apply(
                    n, first * blocks + n, sol[n], gram_high, gram_low, values_w
                ).astype(out_ref.dtype)
            return carry

        for j in range(half):
            finish(j, 0)
        return carry

    lax.fori_loop(0, 2, run, 0)
    for kind in (GRAM, MOMENT):
        for p in range(2):
            to_mate(kind, p).wait_send()
            to_back(kind, p).wait_send()
            for off in range(1, pairs):
                @pl.when(pair + off < pairs)
                def _():
                    to_later(kind, p, off).wait_send()
    for shift in range(1, n_head):
        to_head(shift).wait_send()
    for i in range(2):
        to_plane(i).wait_send()
        to_chip(i).wait()


def project_kernel(readout, w_hbm, pieces_ref, out_ref, weight, result, in_sem, out_sems):
    count, tokens, width = result.shape
    depth = readout.shape[1]
    rows = tokens // out_sems.shape[1]
    me = lax.axis_index("head")
    own = w_hbm.at[pl.ds(pl.multiple_of(me * depth, depth), depth)]
    fetch = pltpu.make_async_copy(own, weight, in_sem)
    fetch.start()
    stores = []
    for shift in (*range(1, count), 0):
        if shift:
            piece = pieces_ref[shift - 1].reshape(depth, width)
        else:
            fetch.wait()
            piece = weight[...]
        owner = lax.rem(me + count - shift, count)
        columns = pl.ds(pl.multiple_of(owner * width, width), width)
        for block in range(tokens // rows):
            part = pl.ds(block * rows, rows)
            result[shift, part] = dot(readout[part], piece).astype(result.dtype)
            stores.append(
                pltpu.make_async_copy(
                    result.at[shift, part], out_ref.at[0, part, columns], out_sems.at[shift, block]
                )
            )
            stores[-1].start()
    for store in stores:
        store.wait()


def shards(n_seq, n_head, queries, keys, values, gates, ridge, out_weight):
    tokens, head_width = queries.shape
    heads = head_width // HD
    half = heads // 2
    blocks = tokens // SPAN
    pairs = n_seq // 2
    width = out_weight.shape[1]
    tile = SPAN * HD * HD * 2
    hbm = pl.BlockSpec(memory_space=pl.ANY)
    in_vmem = pl.BlockSpec(memory_space=pltpu.VMEM)

    def square(*lead, dtype=f32):
        return pltpu.VMEM((*lead, HD, HD), dtype)

    def strip(*lead, dtype=f32):
        return pltpu.VMEM((*lead, HD // 2, HD), dtype)

    every, some = heads * blocks, half * blocks
    readout, pieces = pl.pallas_call(
        functools.partial(solve_kernel, n_seq, n_head),
        in_specs=[hbm, hbm, hbm, in_vmem, pl.BlockSpec(memory_space=pltpu.SMEM), hbm],
        out_specs=[in_vmem, in_vmem],
        out_shape=[
            pltpu.VMEM((tokens, head_width), bf16),
            pltpu.VMEM((n_head - 1, 2, 4, head_width // 8, width), bf16),
        ],
        scratch_shapes=[
            *[pltpu.VMEM((tokens, head_width), bf16)] * 3,
            pltpu.VMEM((tokens, heads), f32),
            *[square(every, dtype=bf16)] * 3,
            *[square(every)] * 3,
            *[square(some, dtype=bf16)] * 2,
            *[square(some)] * 5,
            square(2, heads),
            strip(2, 2, half), strip(2, half), strip(2, half, dtype=bf16),
            strip(2, pairs - 1, half), strip(2, pairs - 1, half, dtype=bf16),
            strip(2, 2, half), square(2, heads),
            pltpu.SemaphoreType.DMA((4,)),
            pltpu.SemaphoreType.DMA((2, n_head - 1)),
            pltpu.SemaphoreType.DMA((2, 2)),
            pltpu.SemaphoreType.DMA((2, 2)),
            pltpu.SemaphoreType.DMA((2, 2, 2)),
            pltpu.SemaphoreType.DMA((2, 2, pairs - 1)),
            pltpu.SemaphoreType.DMA((2, 2, pairs - 1)),
            pltpu.SemaphoreType.DMA((2, 2, 2)),
        ],
        compiler_params=pltpu.CompilerParams(
            vmem_limit_bytes=VMEM_BYTES, collective_id=0, has_side_effects=True
        ),
        cost_estimate=pl.CostEstimate(
            flops=heads * blocks * 58 * tile, bytes_accessed=tokens * head_width * 8, transcendentals=0
        ),
        name="solve",
    )(keys, values, queries, gates.T, ridge, out_weight)
    return pl.pallas_call(
        project_kernel,
        in_specs=[in_vmem, hbm, in_vmem],
        out_specs=hbm,
        out_shape=jax.ShapeDtypeStruct((1, tokens, width * n_head), bf16),
        scratch_shapes=[
            pltpu.VMEM((head_width, width), bf16),
            pltpu.VMEM((n_head, tokens, width), bf16),
            pltpu.SemaphoreType.DMA(()),
            pltpu.SemaphoreType.DMA((n_head, tokens // PROJECT_ROWS)),
        ],
        compiler_params=pltpu.CompilerParams(vmem_limit_bytes=PROJECT_BYTES),
        cost_estimate=pl.CostEstimate(
            flops=2 * tokens * head_width * width * n_head,
            bytes_accessed=tokens * width * n_head * 2,
            transcendentals=0,
        ),
        name="project",
    )(readout, out_weight, pieces)


def solution(mesh):
    return jax.shard_map(
        functools.partial(shards, mesh.shape["seq"], mesh.shape["head"]),
        mesh=mesh,
        in_specs=(
            P("seq", "head"),
            P("seq", "head"),
            P("seq", "head"),
            P("seq", "head"),
            P("head"),
            P(None, "head"),
        ),
        out_specs=P("head", "seq", None),
        check_vma=False,
    )
```
